128 devices in a mesh: grp: 32 (over y, x, core), col: 4 (over z).
Axes of the slice: x: 4, y: 4, z: 4, core: 2. Of those that a mesh axis runs over, the one named last changes fastest.
Arguments:
- old_tables: bfloat16 [128, 128, 32768], P(('grp', 'col')), may hold values from -3 to 3
- table_rows: int32 [128], replicated, may hold values from 4096 to 32768, as said below
- old_plan: int32 [128], replicated, may hold values from 0 to 127, each once
- new_plan: int32 [128], replicated, may hold values from 0 to 127, each once
- ids: int32 [1024, 128, 16], P(('grp', 'col')), may hold values from 0 to 32767, as said below
- bag_len: int32 [1024, 128], P(('grp', 'col')), may hold values from 1 to 16
Outputs:
- new_tables: bfloat16 [128, 128, 32768], P('grp', 'col')
- pooled: float32 [1024, 128, 128], P(('grp', 'col'))
The draws below stay inside these ranges and needn't reach their ends.
Inputs may be any that keep to these rules, and one draw needn't show every extreme that they name: table_rows[t] is a multiple of 4096, and some table has exactly 32768 rows. `ids`: every id of table t lies below table_rows[t].
All inputs are finite; a program needn't handle non-finite values.
Results may differ from the reference program's by a relative error of at most 0.001.
Values may be sent and summed in bfloat16 or wider, within the bound.
A program may use at most 128 MiB of HBM per device.

```python
import jax
import jax.numpy as jnp
from jax import lax

W = 128
ROWS = 32768
BAG = 16
TABLES = 128
BATCH = 1024


def table_sizes(key):
    base = jax.random.fold_in(key, 7)
    eighths = jax.random.randint(jax.random.fold_in(base, 1), (TABLES,), 1, 9)
    chosen = jax.random.randint(jax.random.fold_in(base, 2), (), 0, TABLES)
    eighths = jnp.where(jnp.arange(TABLES) == chosen, 8, eighths)
    return (eighths * (ROWS // 8)).astype(jnp.int32)


def draw_table_rows(key, part):
    return table_sizes(key)


def draw_ids(key, part):
    limits = table_sizes(key)
    drawn = jax.random.randint(jax.random.fold_in(key, 11), (BATCH, TABLES, BAG), 0, limits[None, :, None])
    return drawn.astype(jnp.int32)


def with_ends(values, own_key, low, largest):
    longest = values.shape.index(max(values.shape))
    spots = []
    for shift in (0, 1):
        where = [jax.random.randint(jax.random.fold_in(own_key, axis), (), 0, length) for axis, length in enumerate(values.shape)]
        where[longest] = (where[longest] + shift) % values.shape[longest]
        spots.append(tuple(where))
    return values.at[spots[0]].set(low).at[spots[1]].set(largest)


def shard_levels(key, dims, shards, smallest, largest):
    def one(dim, parts):
        heights = jax.random.uniform(jax.random.fold_in(jax.random.fold_in(key, 6), dim), (parts,), jnp.float32, smallest / len(shards), largest / len(shards))
        return jnp.repeat(jnp.exp(heights), dims[dim] // parts).reshape((-1,) + (1,) * (len(dims) - dim - 1))

    loudness = one(*shards[0])
    for cut in shards[1:]:
        loudness = loudness * one(*cut)
    return loudness


def centred(stream_key, shape, spread, bound, cuts=(), held_as=jnp.bfloat16):
    result = jax.random.normal(stream_key, shape, jnp.float32) * spread
    if len(cuts) > 0:
        result = shard_levels(stream_key, shape, cuts, -0.22, 0.18) * result
    return jnp.clip(result, min=-bound, max=bound).astype(held_as)


def setup_inputs(seed: int = 0) -> dict:
    splits = jax.random.split(jax.random.key(seed), 7)
    return {
        "old_tables": centred(splits[0], (TABLES, W, ROWS), 0.5, 3.0, ((0, 128),)),
        "table_rows": draw_table_rows(jax.random.fold_in(splits[6], 71), 0),
        "old_plan": jax.random.permutation(splits[2], TABLES).astype(jnp.int32),
        "new_plan": jax.random.permutation(splits[3], TABLES).astype(jnp.int32),
        "ids": draw_ids(jax.random.fold_in(splits[6], 71), 0),
        "bag_len": with_ends(jax.random.randint(splits[5], (BATCH, TABLES), 1, BAG + 1), jax.random.fold_in(splits[5], 1), 1, BAG).astype(jnp.int32),
    }


def reference(old_tables, table_rows, old_plan, new_plan, ids, bag_len):
    old_inverse = jnp.argsort(old_plan).astype(jnp.int32)
    new_inverse = jnp.argsort(new_plan).astype(jnp.int32)
    row_iota = jnp.arange(ROWS, dtype=jnp.int32)
    bag_iota = jnp.arange(BAG, dtype=jnp.int32)

    def one_table(position):
        table_id = new_plan[position]
        old_slot = old_inverse[table_id]
        stored = lax.dynamic_index_in_dim(old_tables, old_slot, 0, keepdims=False)
        keep_rows = (row_iota < table_rows[table_id]).astype(old_tables.dtype)
        masked = stored * keep_rows[None, :]
        table_ids = lax.dynamic_index_in_dim(ids, table_id, 1, keepdims=False)
        lengths = lax.dynamic_index_in_dim(bag_len, table_id, 1, keepdims=False)
        values = jnp.take(masked, table_ids, axis=1).astype(jnp.float32)
        in_bag = (bag_iota[None, :] < lengths[:, None]).astype(jnp.float32)
        sums = jnp.sum(values * in_bag[None, :, :], axis=2)
        return masked, sums

    new_tables, sums = lax.map(one_table, jnp.arange(TABLES, dtype=jnp.int32))
    pooled = jnp.transpose(sums[new_inverse], (2, 0, 1))
    return new_tables, pooled
```

```python
import functools

import jax
import jax.numpy as jnp
from jax import lax
from jax.experimental import pallas as pl
from jax.experimental.pallas import tpu as pltpu
from jax.sharding import PartitionSpec as P

MESH = pl.DeviceIdType.MESH
LANES = 128
UNIT = 4096


def invert(permutation):
    entries = permutation.shape[0]
    across = lax.broadcasted_iota(jnp.int32, (entries, entries), 1)
    down = lax.broadcasted_iota(jnp.int32, (entries, entries), 0)
    return jnp.sum(jnp.where(permutation[None, :] == down, across, 0), axis=1)


def pool_rows(table_cols, marked):
    columns = table_cols.shape[0]
    safe_ids = jnp.maximum(marked, 0).reshape(-1)
    weights = (marked >= 0).astype(jnp.float32)
    picked = (
        jnp.take(table_cols, safe_ids, axis=1)
        .reshape(columns, marked.shape[0], marked.shape[1])
        .astype(jnp.float32)
    )
    return jnp.sum(picked * weights[None, :, :], axis=2)


def place(index):
    core = lax.rem(index, 2)
    x = lax.rem(lax.div(index, 2), 4)
    y = lax.rem(lax.div(index, 8), 4)
    z = lax.div(index, 32)
    return y, x, core, z


def peer_of(offset, me):
    dy, dx, dc, dz = place(offset)
    y, x, core, z = me
    ty, tx = lax.rem(y + dy, 4), lax.rem(x + dx, 4)
    tc, tz = lax.rem(core + dc, 2), lax.rem(z + dz, 4)
    return (ty * 4 + tx) * 2 + tc, tz


def exchange_kernel(
    groups, cols, stride, slots_ref, units_ref, table_ref, out_ref,
    blocks, landed, packed, local_sem, send_sem, recv_sem, send2_sem, recv2_sem,
):
    devices = groups * cols
    width = table_ref.shape[1]
    narrow = width // cols
    column_blocks = table_ref.shape[2] // LANES
    units = column_blocks // groups
    grp = lax.axis_index("grp")
    col = lax.axis_index("col")
    own = grp * cols + col
    me = (lax.div(grp, 8), lax.rem(lax.div(grp, 2), 4), lax.rem(grp, 2), col)

    def load(j, carry):
        pltpu.make_async_copy(
            table_ref.at[0, :, pl.ds(pl.multiple_of(j * LANES, LANES), LANES)],
            blocks.at[lax.div(j, groups), lax.rem(j, groups)],
            local_sem,
        ).start()
        return carry

    lax.fori_loop(0, column_blocks, load, 0)
    pltpu.make_async_copy(blocks, blocks, local_sem).wait()

    def send(i, carry):
        offset = lax.rem(i * stride, devices)
        to_grp, to_col = peer_of(offset, me)
        pltpu.make_async_remote_copy(
            src_ref=blocks.at[:, to_grp, pl.ds(pl.multiple_of(to_col * narrow, narrow), narrow), :],
            dst_ref=landed.at[own],
            send_sem=send_sem,
            recv_sem=recv_sem,
            device_id=(to_grp, to_col),
            device_id_type=MESH,
        ).start()
        return carry

    lax.fori_loop(1, devices, send, 0)
    landed[own] = blocks[:, grp, pl.ds(pl.multiple_of(col * narrow, narrow), narrow), :]
    everyone = landed.at[pl.ds(0, devices - 1)]
    pltpu.make_async_copy(everyone, everyone, recv_sem).wait()

    per_group = packed.shape[1]

    def pack(j, carry):
        slot = slots_ref[j]
        count = units_ref[j]
        block = landed[slot]
        unit = lax.broadcasted_iota(jnp.int32, block.shape, 0)
        packed[lax.div(j, per_group), lax.rem(j, per_group)] = jnp.where(
            unit < count, block, jnp.zeros_like(block)
        )
        return carry

    lax.fori_loop(0, groups * per_group, pack, 0)

    def send2(i, carry):
        offset = lax.rem(i * 5, groups)
        to_grp, _ = peer_of(offset, me)
        pltpu.make_async_remote_copy(
            src_ref=packed.at[to_grp],
            dst_ref=out_ref.at[grp],
            send_sem=send2_sem,
            recv_sem=recv2_sem,
            device_id=(to_grp, col),
            device_id_type=MESH,
        ).start()
        return carry

    lax.fori_loop(1, groups, send2, 0)
    mine = pltpu.make_async_copy(packed.at[grp], out_ref.at[grp], local_sem)
    mine.start()
    mine.wait()
    pltpu.make_async_copy(everyone, everyone, send_sem).wait()
    others = packed.at[pl.ds(0, groups - 1)]
    pltpu.make_async_copy(others, others, send2_sem).wait()
    pltpu.make_async_copy(out_ref.at[pl.ds(0, groups - 1)], out_ref.at[pl.ds(0, groups - 1)], recv2_sem).wait()


def exchange(slots, counts, old_tables, groups, cols, stride=37):
    _, width, table_len = old_tables.shape
    devices = groups * cols
    narrow = width // cols
    per_group = slots.shape[0] // groups
    column_blocks = table_len // LANES
    units = column_blocks // groups
    dtype = old_tables.dtype
    return pl.pallas_call(
        functools.partial(exchange_kernel, groups, cols, stride),
        out_shape=jax.ShapeDtypeStruct((groups, per_group, units, narrow, LANES), dtype),
        in_specs=[
            pl.BlockSpec(memory_space=pltpu.SMEM),
            pl.BlockSpec(memory_space=pltpu.SMEM),
            pl.BlockSpec(memory_space=pl.ANY),
        ],
        out_specs=pl.BlockSpec(memory_space=pl.ANY),
        scratch_shapes=[
            pltpu.VMEM((units, groups, width, LANES), dtype),
            pltpu.VMEM((devices, units, narrow, LANES), dtype),
            pltpu.VMEM((groups, per_group, units, narrow, LANES), dtype),
            pltpu.SemaphoreType.DMA,
            pltpu.SemaphoreType.DMA,
            pltpu.SemaphoreType.DMA,
            pltpu.SemaphoreType.DMA,
            pltpu.SemaphoreType.DMA,
        ],
        compiler_params=pltpu.CompilerParams(
            has_side_effects=True, vmem_limit_bytes=60 * 1024 * 1024
        ),
        name="exchange",
    )(slots, counts, old_tables)


def unpack_kernel(in_ref, out_ref):
    groups, _, units = in_ref.shape[:3]
    for k in range(units):
        for p in range(groups):
            start = (k * groups + p) * LANES
            out_ref[0, :, start : start + LANES] = in_ref[p, 0, k]


def unpack(received, step=2):
    groups, per_group, units, narrow, lanes = received.shape
    return pl.pallas_call(
        unpack_kernel,
        out_shape=jax.ShapeDtypeStruct((per_group, narrow, units * groups * lanes), received.dtype),
        grid=(per_group, units // step),
        in_specs=[pl.BlockSpec((groups, 1, step, narrow, lanes), lambda q, k: (0, q, k, 0, 0))],
        out_specs=pl.BlockSpec((1, narrow, step * groups * lanes), lambda q, k: (q, 0, k)),
        name="unpack",
    )(received)


def body(old_tables, table_rows, old_plan, new_plan, ids, bag_len):
    group_count = lax.axis_size("grp")
    col_count = lax.axis_size("col")
    full_width = old_tables.shape[1]
    bag_size = ids.shape[2]
    old_inverse = invert(old_plan)
    slots = old_inverse[new_plan]
    counts = table_rows[new_plan] // UNIT
    received = exchange(slots, counts, old_tables, group_count, col_count)
    new_local = unpack(received)

    bag_iota = lax.broadcasted_iota(jnp.int32, (1, 1, bag_size), 2)
    marked = jnp.where(bag_iota < bag_len[:, :, None], ids, -1)
    by_slot = jnp.take(marked, old_plan, axis=1)
    own_ids = lax.all_to_all(
        by_slot, ("grp", "col"), split_axis=1, concat_axis=0, tiled=True
    ).reshape(-1, bag_size)
    partial_value = pool_rows(old_tables[0], own_ids)
    returned = lax.all_to_all(
        partial_value.reshape(1, full_width, -1),
        ("grp", "col"),
        split_axis=2,
        concat_axis=0,
        tiled=True,
    )
    by_table = jnp.take(returned, old_inverse, axis=0)
    pooled = jnp.transpose(by_table, (2, 0, 1))
    return (new_local, pooled)


def solution(mesh):
    return jax.shard_map(
        body,
        mesh=mesh,
        in_specs=(
            P(("grp", "col"), None, None),
            P(),
            P(),
            P(),
            P(("grp", "col"), None, None),
            P(("grp", "col"), None),
        ),
        out_specs=(P("grp", "col", None), P(("grp", "col"), None, None)),
        check_vma=False,
    )
```

```python
import functools

import jax
import jax.numpy as jnp
from jax import lax
from jax.experimental import pallas as pl
from jax.experimental.pallas import tpu as pltpu
from jax.sharding import PartitionSpec as P

MESH = pl.DeviceIdType.MESH
LANES = 128
UNIT = 4096
BAG = 16


def invert(permutation):
    entries = permutation.shape[0]
    across = lax.broadcasted_iota(jnp.int32, (entries, entries), 1)
    down = lax.broadcasted_iota(jnp.int32, (entries, entries), 0)
    return jnp.sum(jnp.where(permutation[None, :] == down, across, 0), axis=1)


def place(index):
    core = lax.rem(index, 2)
    x = lax.rem(lax.div(index, 2), 4)
    y = lax.rem(lax.div(index, 8), 4)
    z = lax.div(index, 32)
    return y, x, core, z


def peer_of(offset, me):
    dy, dx, dc, dz = place(offset)
    y, x, core, z = me
    ty, tx = lax.rem(y + dy, 4), lax.rem(x + dx, 4)
    tc, tz = lax.rem(core + dc, 2), lax.rem(z + dz, 4)
    return (ty * 4 + tx) * 2 + tc, tz


def exchange_kernel(
    groups, cols, stride, slots_ref, units_ref, ids_ref, table_ref, out_ref, ret_ref,
    blocks, landed, packed, rows_by_id, ids_in, ids_smem, sums,
    local_sem, send_sem, recv_sem, send2_sem, recv2_sem,
    ids_send_sem, ids_recv_sem, sum_send_sem, sum_recv_sem,
):
    devices = groups * cols
    width = table_ref.shape[1]
    narrow = width // cols
    column_blocks = table_ref.shape[2] // LANES
    units = column_blocks // groups
    grp = lax.axis_index("grp")
    col = lax.axis_index("col")
    own = grp * cols + col
    me = (lax.div(grp, 8), lax.rem(lax.div(grp, 2), 4), lax.rem(grp, 2), col)

    def load(j, carry):
        pltpu.make_async_copy(
            table_ref.at[0, :, pl.ds(pl.multiple_of(j * LANES, LANES), LANES)],
            blocks.at[lax.div(j, groups), lax.rem(j, groups)],
            local_sem,
        ).start()
        return carry

    lax.fori_loop(0, column_blocks, load, 0)

    def send_ids(i, carry):
        to_grp, to_col = peer_of(lax.rem(i * stride, devices), me)
        pltpu.make_async_remote_copy(
            src_ref=ids_ref.at[to_grp * cols + to_col],
            dst_ref=ids_in.at[own],
            send_sem=ids_send_sem,
            recv_sem=ids_recv_sem,
            device_id=(to_grp, to_col),
            device_id_type=MESH,
        ).start()
        return carry

    lax.fori_loop(1, devices, send_ids, 0)
    ids_in[own] = ids_ref[own]
    pltpu.make_async_copy(blocks, blocks, local_sem).wait()

    def send(i, carry):
        offset = lax.rem(i * stride, devices)
        to_grp, to_col = peer_of(offset, me)
        pltpu.make_async_remote_copy(
            src_ref=blocks.at[:, to_grp, pl.ds(pl.multiple_of(to_col * narrow, narrow), narrow), :],
            dst_ref=landed.at[own],
            send_sem=send_sem,
            recv_sem=recv_sem,
            device_id=(to_grp, to_col),
            device_id_type=MESH,
        ).start()
        return carry

    lax.fori_loop(1, devices, send, 0)
    landed[own] = blocks[:, grp, pl.ds(pl.multiple_of(col * narrow, narrow), narrow), :]

    table_len = column_blocks * LANES

    def turn(j, carry):
        block = blocks[lax.div(j, groups), lax.rem(j, groups)].astype(jnp.float32)
        rows_by_id[pl.ds(pl.multiple_of(j * LANES, LANES), LANES), :] = block.T
        return carry

    lax.fori_loop(0, column_blocks, turn, 0)
    rows_by_id[pl.ds(table_len, 8), :] = jnp.zeros((8, width), jnp.float32)
    others_ids = ids_in.at[pl.ds(0, devices - 1)]
    pltpu.make_async_copy(others_ids, others_ids, ids_recv_sem).wait()
    to_smem = pltpu.make_async_copy(ids_in, ids_smem, local_sem)
    to_smem.start()
    to_smem.wait()
    samples = sums.shape[1]
    bag = LANES // samples

    def pool(d, carry):
        for b in range(samples):
            terms = [rows_by_id[pl.ds(ids_smem[d, 0, b * bag + i], 1), :] for i in range(bag)]
            while len(terms) > 1:
                terms = [terms[k] + terms[k + 1] for k in range(0, len(terms), 2)]
            sums[d, b : b + 1, :] = terms[0]
        return carry

    lax.fori_loop(0, devices, pool, 0)

    def send_sums(i, carry):
        to_grp, to_col = peer_of(lax.rem(i * stride, devices), me)
        pltpu.make_async_remote_copy(
            src_ref=sums.at[to_grp * cols + to_col],
            dst_ref=ret_ref.at[own],
            send_sem=sum_send_sem,
            recv_sem=sum_recv_sem,
            device_id=(to_grp, to_col),
            device_id_type=MESH,
        ).start()
        return carry

    lax.fori_loop(1, devices, send_sums, 0)
    own_sums = pltpu.make_async_copy(sums.at[own], ret_ref.at[own], local_sem)
    own_sums.start()
    own_sums.wait()
    everyone = landed.at[pl.ds(0, devices - 1)]
    pltpu.make_async_copy(everyone, everyone, recv_sem).wait()

    per_group = packed.shape[1]

    def pack(j, carry):
        slot = slots_ref[j]
        count = units_ref[j]
        block = landed[slot]
        unit = lax.broadcasted_iota(jnp.int32, block.shape, 0)
        packed[lax.div(j, per_group), lax.rem(j, per_group)] = jnp.where(
            unit < count, block, jnp.zeros_like(block)
        )
        return carry

    lax.fori_loop(0, groups * per_group, pack, 0)

    def send2(i, carry):
        offset = lax.rem(i * 5, groups)
        to_grp, _ = peer_of(offset, me)
        pltpu.make_async_remote_copy(
            src_ref=packed.at[to_grp],
            dst_ref=out_ref.at[grp],
            send_sem=send2_sem,
            recv_sem=recv2_sem,
            device_id=(to_grp, col),
            device_id_type=MESH,
        ).start()
        return carry

    lax.fori_loop(1, groups, send2, 0)
    mine = pltpu.make_async_copy(packed.at[grp], out_ref.at[grp], local_sem)
    mine.start()
    mine.wait()
    pltpu.make_async_copy(everyone, everyone, send_sem).wait()
    others = packed.at[pl.ds(0, groups - 1)]
    pltpu.make_async_copy(others, others, send2_sem).wait()
    others_out = out_ref.at[pl.ds(0, groups - 1)]
    pltpu.make_async_copy(others_out, others_out, recv2_sem).wait()
    pltpu.make_async_copy(others_ids, others_ids, ids_send_sem).wait()
    others_sums = sums.at[pl.ds(0, devices - 1)]
    pltpu.make_async_copy(others_sums, others_sums, sum_send_sem).wait()
    others_ret = ret_ref.at[pl.ds(0, devices - 1)]
    pltpu.make_async_copy(others_ret, others_ret, sum_recv_sem).wait()


def exchange(slots, counts, ids, old_tables, groups, cols, stride=37):
    _, width, table_len = old_tables.shape
    devices = groups * cols
    narrow = width // cols
    per_group = slots.shape[0] // groups
    column_blocks = table_len // LANES
    units = column_blocks // groups
    dtype = old_tables.dtype
    samples = LANES // BAG
    return pl.pallas_call(
        functools.partial(exchange_kernel, groups, cols, stride),
        out_shape=(
            jax.ShapeDtypeStruct((groups, per_group, units, narrow, LANES), dtype),
            jax.ShapeDtypeStruct((devices, samples, width), jnp.float32),
        ),
        in_specs=[
            pl.BlockSpec(memory_space=pltpu.SMEM),
            pl.BlockSpec(memory_space=pltpu.SMEM),
            pl.BlockSpec(memory_space=pltpu.VMEM),
            pl.BlockSpec(memory_space=pl.ANY),
        ],
        out_specs=(pl.BlockSpec(memory_space=pl.ANY), pl.BlockSpec(memory_space=pl.ANY)),
        scratch_shapes=[
            pltpu.VMEM((units, groups, width, LANES), dtype),
            pltpu.VMEM((devices, units, narrow, LANES), dtype),
            pltpu.VMEM((groups, per_group, units, narrow, LANES), dtype),
            pltpu.VMEM((table_len + 8, width), jnp.float32),
            pltpu.VMEM((devices, 1, LANES), jnp.int32),
            pltpu.SMEM((devices, 1, LANES), jnp.int32),
            pltpu.VMEM((devices, samples, width), jnp.float32),
        ]
        + [pltpu.SemaphoreType.DMA] * 9,
        compiler_params=pltpu.CompilerParams(
            has_side_effects=True, vmem_limit_bytes=60 * 1024 * 1024
        ),
        name="exchange",
    )(slots, counts, ids, old_tables)


def unpack_kernel(in_ref, out_ref):
    groups, _, units = in_ref.shape[:3]
    for k in range(units):
        for p in range(groups):
            start = (k * groups + p) * LANES
            out_ref[0, :, start : start + LANES] = in_ref[p, 0, k]


def unpack(received, step=2):
    groups, per_group, units, narrow, lanes = received.shape
    return pl.pallas_call(
        unpack_kernel,
        out_shape=jax.ShapeDtypeStruct((per_group, narrow, units * groups * lanes), received.dtype),
        grid=(per_group, units // step),
        in_specs=[pl.BlockSpec((groups, 1, step, narrow, lanes), lambda q, k: (0, q, k, 0, 0))],
        out_specs=pl.BlockSpec((1, narrow, step * groups * lanes), lambda q, k: (q, 0, k)),
        name="unpack",
    )(received)


def body(old_tables, table_rows, old_plan, new_plan, ids, bag_len):
    group_count = lax.axis_size("grp")
    col_count = lax.axis_size("col")
    bag_size = ids.shape[2]
    old_inverse = invert(old_plan)
    slots = old_inverse[new_plan]
    counts = table_rows[new_plan] // UNIT
    bag_iota = lax.broadcasted_iota(jnp.int32, (1, 1, bag_size), 2)
    marked = jnp.where(bag_iota < bag_len[:, :, None], ids, old_tables.shape[2])
    by_slot = jnp.take(marked, old_plan, axis=1)
    own_ids = jnp.transpose(by_slot, (1, 0, 2)).reshape(-1, 1, LANES)
    received, returned = exchange(slots, counts, own_ids, old_tables, group_count, col_count)
    new_local = unpack(received)
    by_table = jnp.take(returned, old_inverse, axis=0)
    pooled = jnp.transpose(by_table, (1, 0, 2))
    return (new_local, pooled)


def solution(mesh):
    return jax.shard_map(
        body,
        mesh=mesh,
        in_specs=(
            P(("grp", "col"), None, None),
            P(),
            P(),
            P(),
            P(("grp", "col"), None, None),
            P(("grp", "col"), None),
        ),
        out_specs=(P("grp", "col", None), P(("grp", "col"), None, None)),
        check_vma=False,
    )
```

```python
import functools

import jax
import jax.numpy as jnp
from jax import lax
from jax.experimental import pallas as pl
from jax.experimental.pallas import tpu as pltpu
from jax.sharding import PartitionSpec as P

MESH = pl.DeviceIdType.MESH
LANES = 128
UNIT = 4096
BAG = 16
ROWS = 32768


def place(index):
    core = lax.rem(index, 2)
    x = lax.rem(lax.div(index, 2), 4)
    y = lax.rem(lax.div(index, 8), 4)
    z = lax.div(index, 32)
    return y, x, core, z


def peer_of(offset, me):
    dy, dx, dc, dz = place(offset)
    y, x, core, z = me
    ty, tx = lax.rem(y + dy, 4), lax.rem(x + dx, 4)
    tc, tz = lax.rem(core + dc, 2), lax.rem(z + dz, 4)
    return (ty * 4 + tx) * 2 + tc, tz


def exchange_kernel(
    groups, cols, stride, slots_ref, units_ref, ids_ref, table_ref, out_ref, ret_ref,
    blocks, landed, packed, rows_by_id, ids_in, ids_smem, sums,
    local_sem, send_sem, recv_sem, send2_sem, recv2_sem,
    ids_send_sem, ids_recv_sem, sum_send_sem, sum_recv_sem,
):
    devices = groups * cols
    width = table_ref.shape[1]
    narrow = width // cols
    column_blocks = table_ref.shape[2] // LANES
    units = column_blocks // groups
    grp = lax.axis_index("grp")
    col = lax.axis_index("col")
    own = grp * cols + col
    me = (lax.div(grp, 8), lax.rem(lax.div(grp, 2), 4), lax.rem(grp, 2), col)

    barrier = pltpu.get_barrier_semaphore()

    def greet(i, carry):
        to_grp, to_col = peer_of(i, me)
        pl.semaphore_signal(barrier, inc=1, device_id=(to_grp, to_col), device_id_type=MESH)
        return carry

    lax.fori_loop(1, devices, greet, 0)

    def load(j, carry):
        pltpu.make_async_copy(
            table_ref.at[0, :, pl.ds(pl.multiple_of(j * LANES, LANES), LANES)],
            blocks.at[lax.div(j, groups), lax.rem(j, groups)],
            local_sem,
        ).start()
        return carry

    lax.fori_loop(0, column_blocks, load, 0)
    pl.semaphore_wait(barrier, devices - 1)

    def send_ids(i, carry):
        to_grp, to_col = peer_of(lax.rem(i * stride, devices), me)
        pltpu.make_async_remote_copy(
            src_ref=ids_ref.at[to_grp * cols + to_col],
            dst_ref=ids_in.at[own],
            send_sem=ids_send_sem,
            recv_sem=ids_recv_sem,
            device_id=(to_grp, to_col),
            device_id_type=MESH,
        ).start()
        return carry

    lax.fori_loop(1, devices, send_ids, 0)
    ids_in[own] = ids_ref[own]
    pltpu.make_async_copy(blocks, blocks, local_sem).wait()

    def send(i, carry):
        offset = lax.rem(i * stride, devices)
        to_grp, to_col = peer_of(offset, me)
        pltpu.make_async_remote_copy(
            src_ref=blocks.at[:, to_grp, pl.ds(pl.multiple_of(to_col * narrow, narrow), narrow), :],
            dst_ref=landed.at[own],
            send_sem=send_sem,
            recv_sem=recv_sem,
            device_id=(to_grp, to_col),
            device_id_type=MESH,
        ).start()
        return carry

    lax.fori_loop(1, devices, send, 0)
    landed[own] = blocks[:, grp, pl.ds(pl.multiple_of(col * narrow, narrow), narrow), :]

    table_len = column_blocks * LANES

    def turn(j, carry):
        for u in range(4):
            p = lax.rem(j, groups // 4) * 4 + u
            unit = lax.div(j, groups // 4)
            start = pl.multiple_of((unit * groups + p) * LANES, LANES)
            rows_by_id[pl.ds(start, LANES), :] = blocks[unit, p].T.astype(jnp.float32)
        return carry

    lax.fori_loop(0, column_blocks // 4, turn, 0)
    rows_by_id[pl.ds(table_len, 8), :] = jnp.zeros((8, width), jnp.float32)
    others_ids = ids_in.at[pl.ds(0, devices - 1)]
    pltpu.make_async_copy(others_ids, others_ids, ids_recv_sem).wait()
    to_smem = pltpu.make_async_copy(ids_in, ids_smem, local_sem)
    to_smem.start()
    to_smem.wait()
    samples = sums.shape[1]
    bag = LANES // samples

    def pool(d, carry):
        for b in range(samples):
            terms = [rows_by_id[pl.ds(ids_smem[d, 0, b * bag + i], 1), :] for i in range(bag)]
            while len(terms) > 1:
                terms = [terms[k] + terms[k + 1] for k in range(0, len(terms), 2)]
            sums[d, b : b + 1, :] = terms[0]
        return carry

    lax.fori_loop(0, devices, pool, 0)

    def send_sums(i, carry):
        to_grp, to_col = peer_of(lax.rem(i * stride, devices), me)
        pltpu.make_async_remote_copy(
            src_ref=sums.at[to_grp * cols + to_col],
            dst_ref=ret_ref.at[own],
            send_sem=sum_send_sem,
            recv_sem=sum_recv_sem,
            device_id=(to_grp, to_col),
            device_id_type=MESH,
        ).start()
        return carry

    lax.fori_loop(1, devices, send_sums, 0)
    own_sums = pltpu.make_async_copy(sums.at[own], ret_ref.at[own], local_sem)
    own_sums.start()
    own_sums.wait()
    everyone = landed.at[pl.ds(0, devices - 1)]
    pltpu.make_async_copy(everyone, everyone, recv_sem).wait()

    per_group = packed.shape[1]

    def pack(j, carry):
        slot = slots_ref[j]
        count = units_ref[j]
        block = landed[slot]
        unit = lax.broadcasted_iota(jnp.int32, block.shape, 0)
        packed[lax.div(j, per_group), lax.rem(j, per_group)] = jnp.where(
            unit < count, block, jnp.zeros_like(block)
        )
        return carry

    lax.fori_loop(0, groups * per_group, pack, 0)

    def send2(i, carry):
        offset = lax.rem(lax.rem(i, groups - 1) + 1, groups) * 27
        q = lax.div(i, groups - 1)
        to_grp, _ = peer_of(lax.rem(offset, groups), me)
        pltpu.make_async_remote_copy(
            src_ref=packed.at[to_grp, q],
            dst_ref=out_ref.at[grp, q],
            send_sem=send2_sem,
            recv_sem=recv2_sem,
            device_id=(to_grp, col),
            device_id_type=MESH,
        ).start()
        return carry

    lax.fori_loop(0, per_group * (groups - 1), send2, 0)
    mine = pltpu.make_async_copy(packed.at[grp], out_ref.at[grp], local_sem)
    mine.start()
    mine.wait()
    pltpu.make_async_copy(everyone, everyone, send_sem).wait()
    others = packed.at[pl.ds(0, groups - 1)]
    pltpu.make_async_copy(others, others, send2_sem).wait()
    others_out = out_ref.at[pl.ds(0, groups - 1)]
    pltpu.make_async_copy(others_out, others_out, recv2_sem).wait()
    pltpu.make_async_copy(others_ids, others_ids, ids_send_sem).wait()
    others_sums = sums.at[pl.ds(0, devices - 1)]
    pltpu.make_async_copy(others_sums, others_sums, sum_send_sem).wait()
    others_ret = ret_ref.at[pl.ds(0, devices - 1)]
    pltpu.make_async_copy(others_ret, others_ret, sum_recv_sem).wait()


def exchange(slots, counts, ids, old_tables, groups, cols, stride=37):
    _, width, table_len = old_tables.shape
    devices = groups * cols
    narrow = width // cols
    per_group = slots.shape[0] // groups
    column_blocks = table_len // LANES
    units = column_blocks // groups
    dtype = old_tables.dtype
    samples = LANES // BAG
    return pl.pallas_call(
        functools.partial(exchange_kernel, groups, cols, stride),
        out_shape=(
            jax.ShapeDtypeStruct((groups, per_group, units, narrow, LANES), dtype),
            jax.ShapeDtypeStruct((devices, samples, width), jnp.float32),
        ),
        in_specs=[
            pl.BlockSpec(memory_space=pltpu.SMEM),
            pl.BlockSpec(memory_space=pltpu.SMEM),
            pl.BlockSpec(memory_space=pltpu.VMEM),
            pl.BlockSpec(memory_space=pl.ANY),
        ],
        out_specs=(pl.BlockSpec(memory_space=pl.ANY), pl.BlockSpec(memory_space=pl.ANY)),
        scratch_shapes=[
            pltpu.VMEM((units, groups, width, LANES), dtype),
            pltpu.VMEM((devices, units, narrow, LANES), dtype),
            pltpu.VMEM((groups, per_group, units, narrow, LANES), dtype),
            pltpu.VMEM((table_len + 8, width), jnp.float32),
            pltpu.VMEM((devices, 1, LANES), jnp.int32),
            pltpu.SMEM((devices, 1, LANES), jnp.int32),
            pltpu.VMEM((devices, samples, width), jnp.float32),
        ]
        + [pltpu.SemaphoreType.DMA] * 9,
        compiler_params=pltpu.CompilerParams(
            collective_id=0, has_side_effects=True, vmem_limit_bytes=60 * 1024 * 1024
        ),
        name="exchange",
    )(slots, counts, ids, old_tables)


def plan_kernel(devices, old_ref, new_ref, rows_ref, ids_ref, len_ref, slots_ref, counts_ref, inv_ref, ids_out, turned):
    def invert(s, carry):
        inv_ref[old_ref[s]] = s
        return carry

    lax.fori_loop(0, devices, invert, 0)

    def place_of(j, carry):
        table = new_ref[j]
        slots_ref[j] = inv_ref[table]
        counts_ref[j] = lax.div(rows_ref[table], UNIT)
        return carry

    lax.fori_loop(0, devices, place_of, 0)
    samples, tables = len_ref.shape
    turn_in = lax.broadcasted_iota(jnp.int32, (BAG, tables), 0)
    parts = []
    for b in range(samples):
        used = turn_in < len_ref[b : b + 1, :]
        parts.append(jnp.where(used, ids_ref[b * BAG : (b + 1) * BAG, :], ROWS))
    turned[...] = jnp.concatenate(parts, axis=0).T

    def pick(s, carry):
        for u in range(8):
            ids_out[s * 8 + u] = turned[pl.ds(old_ref[s * 8 + u], 1), :]
        return carry

    lax.fori_loop(0, devices // 8, pick, 0)


def plan(old_plan, new_plan, table_rows, ids, bag_len):
    tables = old_plan.shape[0]
    smem = pl.BlockSpec(memory_space=pltpu.SMEM)
    vmem = pl.BlockSpec(memory_space=pltpu.VMEM)
    small = jax.ShapeDtypeStruct((tables,), jnp.int32)
    flat = jnp.transpose(ids, (0, 2, 1)).reshape(-1, tables)
    return pl.pallas_call(
        functools.partial(plan_kernel, tables),
        out_shape=(small, small, small, jax.ShapeDtypeStruct((tables, 1, flat.shape[0]), jnp.int32)),
        in_specs=[smem, smem, smem, vmem, vmem],
        out_specs=(smem, smem, smem, vmem),
        scratch_shapes=[pltpu.VMEM((tables, flat.shape[0]), jnp.int32)],
        name="plan",
    )(old_plan, new_plan, table_rows, flat, bag_len)


def unpack_kernel(step, inv_ref, in_ref, ret_ref, out_ref, pooled_ref):
    groups, _, units = in_ref.shape[:3]
    for k in range(units):
        for p in range(groups):
            start = (k * groups + p) * LANES
            out_ref[0, :, start : start + LANES] = in_ref[p, 0, k]
    tables = inv_ref.shape[0]
    samples = pooled_ref.shape[0]
    share = tables // step
    first = (pl.program_id(0) * pl.num_programs(1) + pl.program_id(1)) * share

    def reorder(i, carry):
        table = first + i
        rows = ret_ref[inv_ref[table]]
        for b in range(samples):
            pooled_ref[b, pl.ds(table, 1), :] = rows[b : b + 1, :]
        return carry

    lax.fori_loop(0, share, reorder, 0)


def unpack(inverse, received, returned, step=4):
    groups, per_group, units, narrow, lanes = received.shape
    devices, samples, width = returned.shape
    grid = (per_group, units // step)
    return pl.pallas_call(
        functools.partial(unpack_kernel, per_group * units // step),
        out_shape=(
            jax.ShapeDtypeStruct((per_group, narrow, units * groups * lanes), received.dtype),
            jax.ShapeDtypeStruct((samples, devices, width), returned.dtype),
        ),
        grid=grid,
        in_specs=[
            pl.BlockSpec(memory_space=pltpu.SMEM),
            pl.BlockSpec((groups, 1, step, narrow, lanes), lambda q, k: (0, q, k, 0, 0)),
            pl.BlockSpec((devices, samples, width), lambda q, k: (0, 0, 0)),
        ],
        out_specs=(
            pl.BlockSpec((1, narrow, step * groups * lanes), lambda q, k: (q, 0, k)),
            pl.BlockSpec((samples, devices, width), lambda q, k: (0, 0, 0)),
        ),
        compiler_params=pltpu.CompilerParams(vmem_limit_bytes=40 * 1024 * 1024),
        name="unpack",
    )(inverse, received, returned)


def body(old_tables, table_rows, old_plan, new_plan, ids, bag_len):
    group_count = lax.axis_size("grp")
    col_count = lax.axis_size("col")
    slots, counts, inverse, own_ids = plan(old_plan, new_plan, table_rows, ids, bag_len)
    received, returned = exchange(slots, counts, own_ids, old_tables, group_count, col_count)
    return unpack(inverse, received, returned)


def solution(mesh):
    return jax.shard_map(
        body,
        mesh=mesh,
        in_specs=(
            P(("grp", "col"), None, None),
            P(),
            P(),
            P(),
            P(("grp", "col"), None, None),
            P(("grp", "col"), None),
        ),
        out_specs=(P("grp", "col", None), P(("grp", "col"), None, None)),
        check_vma=False,
    )
```

```python
import functools

import jax
import jax.numpy as jnp
from jax import lax
from jax.experimental import pallas as pl
from jax.experimental.pallas import tpu as pltpu
from jax.sharding import PartitionSpec as P

MESH = pl.DeviceIdType.MESH
LANES = 128
UNIT = 4096
BAG = 16
ROWS = 32768
CHUNKS = 4
ORDER = ((1, 0), (1, 1), (0, 0), (2, 0), (1, 2), (2, 1), (3, 0), (1, 3), (2, 2), (3, 1), (2, 3), (3, 2), (3, 3))
HOLD = 88
LEVELS = ((60, 27), (64, 29), (72, 31), (88, 32))
LEVELS_ID = len(LEVELS)
LISTS3, SLOTS, COUNTS, INVERSE, MINE, LEVEL = 8, 24, 25, 26, 27, 28


def place(index):
    core = lax.rem(index, 2)
    x = lax.rem(lax.div(index, 2), 4)
    y = lax.rem(lax.div(index, 8), 4)
    z = lax.div(index, 32)
    return y, x, core, z


def peer_of(offset, me):
    dy, dx, dc, dz = place(offset)
    y, x, core, z = me
    ty, tx = lax.rem(y + dy, 4), lax.rem(x + dx, 4)
    tc, tz = lax.rem(core + dc, 2), lax.rem(z + dz, 4)
    return (ty * 4 + tx) * 2 + tc, tz


def greet_all(groups, cols, me):
    barrier = pltpu.get_barrier_semaphore()

    def greet(i, carry):
        to_grp, to_col = peer_of(i, me)
        pl.semaphore_signal(barrier, inc=1, device_id=(to_grp, to_col), device_id_type=MESH)
        return carry

    lax.fori_loop(1, groups * cols, greet, 0)
    return barrier


def load_table(groups, table_ref, blocks, sem):
    def load(j, carry):
        pltpu.make_async_copy(
            table_ref.at[0, :, pl.ds(pl.multiple_of(j * LANES, LANES), LANES)],
            blocks.at[lax.div(j, groups), lax.rem(j, groups)],
            sem,
        ).start()
        return carry

    lax.fori_loop(0, table_ref.shape[2] // LANES, load, 0)


def send_rows(groups, cols, stride, me, own, source, target, send_sem, recv_sem):
    devices = groups * cols

    def send(i, carry):
        to_grp, to_col = peer_of(lax.rem(i * stride, devices), me)
        pltpu.make_async_remote_copy(
            src_ref=source.at[to_grp * cols + to_col],
            dst_ref=target.at[own],
            send_sem=send_sem,
            recv_sem=recv_sem,
            device_id=(to_grp, to_col),
            device_id_type=MESH,
        ).start()
        return carry

    lax.fori_loop(1, devices, send, 0)


def pool_bags(groups, cols, blocks, rows_by_id, ids_in, ids_smem, sums, ids_recv_sem, local_sem):
    devices = groups * cols
    units, _, width, _ = blocks.shape
    table_len = units * groups * LANES

    def turn(j, carry):
        for u in range(4):
            p = lax.rem(j, groups // 4) * 4 + u
            unit = lax.div(j, groups // 4)
            start = pl.multiple_of((unit * groups + p) * LANES, LANES)
            rows_by_id[pl.ds(start, LANES), :] = blocks[unit, p].T.astype(jnp.float32)
        return carry

    lax.fori_loop(0, units * groups // 4, turn, 0)
    rows_by_id[pl.ds(table_len, 8), :] = jnp.zeros((8, width), jnp.float32)
    wait_for(ids_in.at[pl.ds(0, devices - 1)], ids_recv_sem)
    to_smem = pltpu.make_async_copy(ids_in, ids_smem, local_sem)
    to_smem.start()
    to_smem.wait()
    samples = sums.shape[1]

    def pool(d, carry):
        for b in range(samples):
            terms = [rows_by_id[pl.ds(ids_smem[d, 0, b * BAG + i], 1), :] for i in range(BAG)]
            while len(terms) > 1:
                terms = [terms[k] + terms[k + 1] for k in range(0, len(terms), 2)]
            sums[d, b : b + 1, :] = terms[0]
        return carry

    lax.fori_loop(0, devices, pool, 0)


def wait_for(ref, sem):
    pltpu.make_async_copy(ref, ref, sem).wait()


def exchange_kernel(
    groups, cols, stride, tables_ref, ids_ref, table_ref, out_ref, ret_ref,
    blocks, landed, packed, rows_by_id, ids_in, ids_smem, sums,
    local_sem, send_sem, recv_sem, send2_sem, recv2_sem,
    ids_send_sem, ids_recv_sem, sum_send_sem, sum_recv_sem,
):
    devices = groups * cols
    width = table_ref.shape[1]
    narrow = width // cols
    grp = lax.axis_index("grp")
    col = lax.axis_index("col")
    own = grp * cols + col
    me = (lax.div(grp, 8), lax.rem(lax.div(grp, 2), 4), lax.rem(grp, 2), col)

    barrier = greet_all(groups, cols, me)
    load_table(groups, table_ref, blocks, local_sem)
    pl.semaphore_wait(barrier, devices - 1)
    send_rows(groups, cols, stride, me, own, ids_ref, ids_in, ids_send_sem, ids_recv_sem)
    ids_in[own] = ids_ref[own]
    wait_for(blocks, local_sem)

    def send(i, carry):
        offset = lax.rem(i * stride, devices)
        to_grp, to_col = peer_of(offset, me)
        pltpu.make_async_remote_copy(
            src_ref=blocks.at[:, to_grp, pl.ds(pl.multiple_of(to_col * narrow, narrow), narrow), :],
            dst_ref=landed.at[own],
            send_sem=send_sem,
            recv_sem=recv_sem,
            device_id=(to_grp, to_col),
            device_id_type=MESH,
        ).start()
        return carry

    lax.fori_loop(1, devices, send, 0)
    landed[own] = blocks[:, grp, pl.ds(pl.multiple_of(col * narrow, narrow), narrow), :]

    pool_bags(groups, cols, blocks, rows_by_id, ids_in, ids_smem, sums, ids_recv_sem, local_sem)
    send_rows(groups, cols, stride, me, own, sums, ret_ref, sum_send_sem, sum_recv_sem)
    own_sums = pltpu.make_async_copy(sums.at[own], ret_ref.at[own], local_sem)
    own_sums.start()
    own_sums.wait()
    everyone = landed.at[pl.ds(0, devices - 1)]
    wait_for(everyone, recv_sem)

    per_group = packed.shape[1]

    def pack(j, carry):
        slot = tables_ref[SLOTS, j]
        count = tables_ref[COUNTS, j]
        block = landed[slot]
        unit = lax.broadcasted_iota(jnp.int32, block.shape, 0)
        packed[lax.div(j, per_group), lax.rem(j, per_group)] = jnp.where(
            unit < count, block, jnp.zeros_like(block)
        )
        return carry

    lax.fori_loop(0, groups * per_group, pack, 0)

    def send2(i, carry):
        offset = lax.rem(lax.rem(i, groups - 1) + 1, groups) * 27
        q = lax.div(i, groups - 1)
        to_grp, _ = peer_of(lax.rem(offset, groups), me)
        pltpu.make_async_remote_copy(
            src_ref=packed.at[to_grp, q],
            dst_ref=out_ref.at[grp, q],
            send_sem=send2_sem,
            recv_sem=recv2_sem,
            device_id=(to_grp, col),
            device_id_type=MESH,
        ).start()
        return carry

    lax.fori_loop(0, per_group * (groups - 1), send2, 0)
    mine = pltpu.make_async_copy(packed.at[grp], out_ref.at[grp], local_sem)
    mine.start()
    mine.wait()
    wait_for(everyone, send_sem)
    wait_for(packed.at[pl.ds(0, groups - 1)], send2_sem)
    wait_for(out_ref.at[pl.ds(0, groups - 1)], recv2_sem)
    wait_for(ids_in.at[pl.ds(0, devices - 1)], ids_send_sem)
    wait_for(sums.at[pl.ds(0, devices - 1)], sum_send_sem)
    wait_for(ret_ref.at[pl.ds(0, devices - 1)], sum_recv_sem)


def exchange(tables, ids, old_tables, groups, cols, stride=37):
    _, width, table_len = old_tables.shape
    devices = groups * cols
    narrow = width // cols
    per_group = tables.shape[1] // groups
    column_blocks = table_len // LANES
    units = column_blocks // groups
    dtype = old_tables.dtype
    samples = LANES // BAG
    return pl.pallas_call(
        functools.partial(exchange_kernel, groups, cols, stride),
        out_shape=(
            jax.ShapeDtypeStruct((groups, per_group, units, narrow, LANES), dtype),
            jax.ShapeDtypeStruct((devices, samples, width), jnp.float32),
        ),
        in_specs=[
            pl.BlockSpec(memory_space=pltpu.SMEM),
            pl.BlockSpec(memory_space=pltpu.VMEM),
            pl.BlockSpec(memory_space=pl.ANY),
        ],
        out_specs=(pl.BlockSpec(memory_space=pl.ANY), pl.BlockSpec(memory_space=pl.ANY)),
        scratch_shapes=[
            pltpu.VMEM((units, groups, width, LANES), dtype),
            pltpu.VMEM((devices, units, narrow, LANES), dtype),
            pltpu.VMEM((groups, per_group, units, narrow, LANES), dtype),
            pltpu.VMEM((table_len + 8, width), jnp.float32),
            pltpu.VMEM((devices, 1, LANES), jnp.int32),
            pltpu.SMEM((devices, 1, LANES), jnp.int32),
            pltpu.VMEM((devices, samples, width), jnp.float32),
        ]
        + [pltpu.SemaphoreType.DMA] * 9,
        compiler_params=pltpu.CompilerParams(
            collective_id=LEVELS_ID, has_side_effects=True, vmem_limit_bytes=60 * 1024 * 1024
        ),
        name="exchange",
    )(tables, ids, old_tables)


def route_kernel(
    groups, cols, stride, cap2, cap3, hold, chunks,
    tables_ref, ids_ref, table_ref, out_ref, ret_ref,
    blocks, rows_by_id, ids_in, ids_smem, sums, first, outgoing, second, final,
    local_sem, ids_send_sem, ids_recv_sem, sum_send_sem, sum_recv_sem,
    send1_sem, recv1_sem, send2_sem, recv2_sem, send3_sem, recv3_sem, own3_sem,
):
    devices = groups * cols
    width = blocks.shape[2]
    narrow = width // cols
    piece = first[0].shape[1]
    parts = narrow // piece
    grp = lax.axis_index("grp")
    col = lax.axis_index("col")
    own = grp * cols + col
    y, x, core = lax.div(grp, 8), lax.rem(lax.div(grp, 2), 4), lax.rem(grp, 2)
    me = (y, x, core, col)
    along = (y, x)
    across = (x, y)
    line = 8
    source = [(along[h] * 2 + core) * cols + col for h in range(2)]
    seat = [along[h] * 2 + core for h in range(2)]

    def at(h, u, v, c):
        return ((u * 4 + v) * 2 + c) if h == 0 else ((v * 4 + u) * 2 + c)

    barrier = greet_all(groups, cols, me)
    load_table(groups, table_ref, blocks, local_sem)
    pl.semaphore_wait(barrier, devices - 1)
    send_rows(groups, cols, stride, me, own, ids_ref, ids_in, ids_send_sem, ids_recv_sem)
    ids_in[own] = ids_ref[own]
    wait_for(blocks, local_sem)

    def stage1(n):
        c, w = n // parts, n % parts

        def send(i, carry):
            o = lax.rem(i * 5, 32)
            dc, du, dz = lax.rem(o, 2), lax.rem(lax.div(o, 2), 4), lax.div(o, 8)
            tz = lax.rem(col + dz, 4)
            tc = lax.rem(core + dc, 2)
            start = pl.multiple_of(tz * narrow + w * piece, piece)
            for h in range(2):
                tu = lax.rem(along[h] + du, 4)
                pltpu.make_async_remote_copy(
                    src_ref=blocks.at[:, h * 16 + c * 8 + tu * 2 + tc, pl.ds(start, piece), :],
                    dst_ref=first[h * chunks + n].at[pl.ds(source[h] * 8, 8)],
                    send_sem=send1_sem.at[h * chunks + n],
                    recv_sem=recv1_sem.at[h * chunks + n],
                    device_id=(at(h, tu, across[h], tc), tz),
                    device_id_type=MESH,
                ).start()
            return carry

        lax.fori_loop(1, 32, send, 0)
        start = pl.multiple_of(col * narrow + w * piece, piece)
        for h in range(2):
            first[h * chunks + n][pl.ds(source[h] * 8, 8)] = blocks[
                :, h * 16 + c * 8 + seat[h], pl.ds(start, piece), :
            ]

    def stage2(n):
        for h in range(2):
            i = h * chunks + n
            wait_for(first[i].at[pl.ds(0, 31 * 8)], recv1_sem.at[i])

            def keep(m, carry):
                for u in range(4):
                    second[i][m * 4 + u] = first[i][tables_ref[h * 4, m * 4 + u]]
                return carry

            lax.fori_loop(0, hold // 4, keep, 0)

            def pack(m, carry):
                for dv in range(1, 4):
                    for u in range(4):
                        outgoing[i][(dv - 1) * cap2 + m * 4 + u] = first[i][
                            tables_ref[h * 4 + dv, m * 4 + u]
                        ]
                return carry

            lax.fori_loop(0, cap2 // 4, pack, 0)
        half = cap2 // 2
        for m in range(2):
            for dv in (1, 3, 2):
                for h in range(2):
                    i = h * chunks + n
                    pltpu.make_async_remote_copy(
                        src_ref=outgoing[i].at[pl.ds((dv - 1) * cap2 + m * half, half)],
                        dst_ref=second[i].at[pl.ds(dv * hold + m * half, half)],
                        send_sem=send2_sem.at[i],
                        recv_sem=recv2_sem.at[i],
                        device_id=(at(h, along[h], lax.rem(across[h] + dv, 4), core), col),
                        device_id_type=MESH,
                    ).start()

    def stage3(n):
        for h in range(2):
            i = h * chunks + n
            wait_for(second[i].at[pl.ds(0, 3 * cap2)], recv2_sem.at[i])

            def pack(m, carry):
                for d in range(line):
                    final[i][d, m] = second[i][tables_ref[LISTS3 + h * line + d, m]]
                return carry

            lax.fori_loop(0, cap3, pack, 0)
        for d in (5, 3, 7, 2, 6, 4, 1):
            for h in range(2):
                i = h * chunks + n
                tu = lax.rem(along[h] + d // 2, 4)
                tc = lax.rem(core + d % 2, 2)
                pltpu.make_async_remote_copy(
                    src_ref=final[i].at[d],
                    dst_ref=out_ref.at[h, n, seat[h]],
                    send_sem=send3_sem.at[i],
                    recv_sem=recv3_sem.at[i],
                    device_id=(at(h, tu, across[h], tc), col),
                    device_id_type=MESH,
                ).start()
        for h in range(2):
            i = h * chunks + n
            pltpu.make_async_copy(final[i].at[0], out_ref.at[h, n, seat[h]], own3_sem.at[i]).start()

    def bags():
        pool_bags(groups, cols, blocks, rows_by_id, ids_in, ids_smem, sums, ids_recv_sem, local_sem)
        send_rows(groups, cols, stride, me, own, sums, ret_ref, sum_send_sem, sum_recv_sem)
        own_sums = pltpu.make_async_copy(sums.at[own], ret_ref.at[own], local_sem)
        own_sums.start()
        own_sums.wait()

    for stage, n in ORDER:
        (bags, stage1, stage2, stage3)[stage](*(n,)[: min(stage, 1)])
    for h in range(2):
        for n in range(chunks):
            i = h * chunks + n
            wait_for(first[i].at[pl.ds(0, 31 * 8)], send1_sem.at[i])
            wait_for(outgoing[i], send2_sem.at[i])
            wait_for(final[i].at[pl.ds(0, line - 1)], send3_sem.at[i])
            wait_for(final[i].at[0], own3_sem.at[i])
            wait_for(out_ref.at[h, n, pl.ds(0, line - 1)], recv3_sem.at[i])
    wait_for(ids_in.at[pl.ds(0, devices - 1)], ids_send_sem)
    wait_for(sums.at[pl.ds(0, devices - 1)], sum_send_sem)
    wait_for(ret_ref.at[pl.ds(0, devices - 1)], sum_recv_sem)


def routed(tables, ids, old_tables, groups, cols, cap2, cap3, number, chunks=CHUNKS, stride=37):
    _, width, table_len = old_tables.shape
    devices = groups * cols
    piece = (width // cols) * 2 // chunks
    units = table_len // LANES // groups
    dtype = old_tables.dtype
    samples = LANES // BAG
    smem = pl.BlockSpec(memory_space=pltpu.SMEM)
    hbm = pl.BlockSpec(memory_space=pl.ANY)
    both = 2 * chunks
    dma = pltpu.SemaphoreType.DMA
    return pl.pallas_call(
        functools.partial(route_kernel, groups, cols, stride, cap2, cap3, HOLD, chunks),
        out_shape=(
            jax.ShapeDtypeStruct((2, chunks, 8, cap3, piece, LANES), dtype),
            jax.ShapeDtypeStruct((devices, samples, width), jnp.float32),
        ),
        in_specs=[smem, pl.BlockSpec(memory_space=pltpu.VMEM), hbm],
        out_specs=(hbm, hbm),
        scratch_shapes=[
            pltpu.VMEM((units, groups, width, LANES), dtype),
            pltpu.VMEM((table_len + 8, width), jnp.float32),
            pltpu.VMEM((devices, 1, LANES), jnp.int32),
            pltpu.SMEM((devices, 1, LANES), jnp.int32),
            pltpu.VMEM((devices, samples, width), jnp.float32),
            [pltpu.VMEM((devices // 4 * units, piece, LANES), dtype) for _ in range(both)],
            [pltpu.VMEM((3 * cap2, piece, LANES), dtype) for _ in range(both)],
            [pltpu.VMEM((4 * HOLD, piece, LANES), dtype) for _ in range(both)],
            [pltpu.VMEM((8, cap3, piece, LANES), dtype) for _ in range(both)],
        ]
        + [dma] * 5
        + [dma((both,))] * 7,
        compiler_params=pltpu.CompilerParams(
            collective_id=number, has_side_effects=True, vmem_limit_bytes=63 * 1024 * 1024
        ),
        name="routed",
    )(tables, ids, old_tables)


def plan_kernel(old_ref, new_ref, rows_ref, ids_ref, len_ref, tables_ref, ids_out, turned):
    samples, size = len_ref.shape
    grp = lax.axis_index("grp")
    y, x, core = lax.div(grp, 8), lax.rem(lax.div(grp, 2), 4), lax.rem(grp, 2)
    down = lax.broadcasted_iota(jnp.int32, (size, size), 0)
    lane = lax.broadcasted_iota(jnp.int32, (size, size), 1)
    index = lax.broadcasted_iota(jnp.int32, (1, size), 1)

    def column(row):
        return jnp.broadcast_to(row, (size, size)).T

    def total(mask, value):
        return jnp.sum(jnp.where(mask, value, 0), axis=0, keepdims=True)

    def put(row, value):
        tables_ref[row : row + 1, :] = value

    old_down = column(old_ref[...])
    new = new_ref[...]
    slot = total(old_down == new, down)
    count = total(down == new, column(rows_ref[...] // UNIT))
    put(SLOTS, slot)
    put(COUNTS, count)
    put(INVERSE, total(old_down == lane, down))
    count_down = column(count)
    target_down = down // 4
    base = total((target_down == index // 4) & (down < lane), count_down)
    base_down = column(base)
    slot_down = column(slot)
    core_from, z_from = (slot_down // 4) % 2, slot_down % 4
    core_to = target_down % 2
    sides = []
    for place_down, place in ((slot_down // 4, slot // 4), (target_down, index // 4)):
        sides.append(((place_down // 8, (place_down // 2) % 4), (place // 8, (place // 2) % 4)))
    need0 = need2 = jnp.zeros((1, 1), jnp.int32)
    for h, (u, v) in enumerate(((y, x), (x, y))):
        u_from, v_from = sides[0][0][h], sides[0][0][1 - h]
        u_to, v_to = sides[1][0][h], sides[1][0][1 - h]
        pair_down = v_from * 4 + v_to
        pair = sides[0][1][1 - h] * 4 + sides[1][1][1 - h]
        begun = total((pair_down == pair) & (down < lane), count_down)
        begun_down = column(begun)
        sums = total(pair_down == lane, count_down)
        same = index % 5 == 0
        need0 = jnp.maximum(need0, jnp.max(jnp.where(same, sums, 0), axis=1, keepdims=True))
        need2 = jnp.maximum(need2, jnp.max(jnp.where(same, 0, sums), axis=1, keepdims=True))
        step = (v_to - v_from + 4) % 4
        source = ((u_from * 2 + core_from) * 4 + z_from) * 8 + lane - begun_down
        inside = (v_from == v) & (lane >= begun_down) & (lane < begun_down + count_down)
        for dv in range(4):
            put(h * 4 + dv, total(inside & (step == dv), source))
        rel = ((u_to - u + 4) % 4) * 2 + (core_to - core + 2) % 2
        held = step * HOLD + jnp.minimum(begun_down + lane - base_down, HOLD - 1)
        inside = (v_to == v) & (lane >= base_down) & (lane < base_down + count_down)
        for d in range(8):
            put(LISTS3 + h * 8 + d, total(inside & (rel == d), held))
    need3 = jnp.max(total(target_down == lane, count_down), axis=1, keepdims=True)
    level = jnp.full((1, 1), len(LEVELS), jnp.int32)
    for number in reversed(range(len(LEVELS))):
        cap2, cap3 = LEVELS[number]
        fits = (need0 <= HOLD) & (need2 <= cap2) & (need3 <= cap3)
        level = jnp.where(fits, number, level)
    put(LEVEL, jnp.broadcast_to(level, (1, size)))
    mine = total(down == grp * 4 + lane, count_down)
    offset = total(down == grp * 4 + lane - 4, base_down)
    put(MINE, jnp.where(index < 4, mine, offset))

    turn_in = lax.broadcasted_iota(jnp.int32, (BAG, size), 0)
    parts = []
    for b in range(samples):
        used = turn_in < len_ref[b : b + 1, :]
        parts.append(jnp.where(used, ids_ref[b * BAG : (b + 1) * BAG, :], ROWS))
    flat = jnp.concatenate(parts, axis=0).T
    high = jnp.dot(
        (old_down == lane).astype(jnp.bfloat16), (flat // 256).astype(jnp.bfloat16),
        preferred_element_type=jnp.float32,
    )
    low = jnp.dot(
        (old_down == lane).astype(jnp.bfloat16), (flat % 256).astype(jnp.bfloat16),
        preferred_element_type=jnp.float32,
    )
    turned[...] = high.astype(jnp.int32) * 256 + low.astype(jnp.int32)

    def copy(s, carry):
        for i in range(8):
            ids_out[s * 8 + i] = turned[pl.ds(s * 8 + i, 1), :]
        return carry

    lax.fori_loop(0, size // 8, copy, 0)


def plan(old_plan, new_plan, table_rows, ids, bag_len):
    tables = old_plan.shape[0]
    vmem = pl.BlockSpec(memory_space=pltpu.VMEM)
    flat = jnp.transpose(ids, (0, 2, 1)).reshape(-1, tables)
    return pl.pallas_call(
        plan_kernel,
        out_shape=(
            jax.ShapeDtypeStruct((32, tables), jnp.int32),
            jax.ShapeDtypeStruct((tables, 1, flat.shape[0]), jnp.int32),
        ),
        in_specs=[vmem] * 5,
        out_specs=(vmem, vmem),
        scratch_shapes=[pltpu.VMEM((tables, flat.shape[0]), jnp.int32)],
        name="plan",
    )(old_plan[None], new_plan[None], table_rows[None], flat, bag_len)


def reorder_sums(share, tables_ref, ret_ref, pooled_ref):
    samples = pooled_ref.shape[0]
    first = (pl.program_id(0) * pl.num_programs(1) + pl.program_id(1)) * share

    def reorder(i, carry):
        table = first + i
        rows = ret_ref[tables_ref[INVERSE, table]]
        for b in range(samples):
            pooled_ref[b, pl.ds(table, 1), :] = rows[b : b + 1, :]
        return carry

    lax.fori_loop(0, share, reorder, 0)


def unpack_kernel(steps, tables_ref, in_ref, ret_ref, out_ref, pooled_ref):
    groups, _, units = in_ref.shape[:3]
    for k in range(units):
        for p in range(groups):
            start = (k * groups + p) * LANES
            out_ref[0, :, start : start + LANES] = in_ref[p, 0, k]
    reorder_sums(tables_ref.shape[1] // steps, tables_ref, ret_ref, pooled_ref)


def unpack_routed_kernel(steps, tables_ref, in_ref, ret_ref, out_ref, pooled_ref):
    halves, chunks, seats, _, piece, lanes = in_ref.shape
    narrow = out_ref.shape[1]
    parts = narrow // piece
    unit = halves * chunks // parts * seats * lanes
    q = pl.program_id(0)
    count, base = tables_ref[MINE, q], tables_ref[MINE, 4 + q]
    for m in range(out_ref.shape[2] // unit):
        k = pl.program_id(1) * (out_ref.shape[2] // unit) + m

        @pl.when(k < count)
        def _():
            for h in range(halves):
                for n in range(chunks):
                    c, w = n // parts, n % parts
                    for p in range(seats):
                        start = m * unit + (h * 16 + c * 8 + p) * lanes
                        out_ref[0, w * piece : (w + 1) * piece, start : start + lanes] = in_ref[
                            h, n, p, base + k
                        ]

        @pl.when(k >= count)
        def _():
            out_ref[0, :, m * unit : (m + 1) * unit] = jnp.zeros((narrow, unit), out_ref.dtype)

    reorder_sums(tables_ref.shape[1] // steps, tables_ref, ret_ref, pooled_ref)


def unpack(kernel, block, index, tables, received, returned, narrow, table_len, step=4):
    devices, samples, width = returned.shape
    per_group = 4
    splits = table_len // UNIT // step
    smem = pl.BlockSpec(memory_space=pltpu.SMEM)
    return pl.pallas_call(
        functools.partial(kernel, per_group * splits),
        out_shape=(
            jax.ShapeDtypeStruct((per_group, narrow, table_len), received.dtype),
            jax.ShapeDtypeStruct((samples, devices, width), returned.dtype),
        ),
        grid=(per_group, splits),
        in_specs=[
            smem,
            pl.BlockSpec(block, index),
            pl.BlockSpec((devices, samples, width), lambda q, k: (0, 0, 0)),
        ],
        out_specs=(
            pl.BlockSpec((1, narrow, step * UNIT), lambda q, k: (q, 0, k)),
            pl.BlockSpec((samples, devices, width), lambda q, k: (0, 0, 0)),
        ),
        compiler_params=pltpu.CompilerParams(vmem_limit_bytes=40 * 1024 * 1024),
        name="unpack",
    )(tables, received, returned)


def body(old_tables, table_rows, old_plan, new_plan, ids, bag_len):
    groups = lax.axis_size("grp")
    cols = lax.axis_size("col")
    _, width, table_len = old_tables.shape
    narrow = width // cols
    tables, own_ids = plan(old_plan, new_plan, table_rows, ids, bag_len)

    def by_level(number):
        cap2, cap3 = LEVELS[number]

        def run():
            received, returned = routed(
                tables, own_ids, old_tables, groups, cols, cap2, cap3, number
            )
            return unpack(
                unpack_routed_kernel, received.shape, lambda q, k: (0,) * 6,
                tables, received, returned, narrow, table_len,
            )

        return run

    def spread():
        received, returned = exchange(tables, own_ids, old_tables, groups, cols)
        block = received.shape[:1] + (1, 4) + received.shape[3:]
        return unpack(
            unpack_kernel, block, lambda q, k: (0, q, k, 0, 0),
            tables, received, returned, narrow, table_len,
        )

    branches = [by_level(number) for number in range(len(LEVELS))] + [spread]
    return lax.switch(tables[LEVEL, 0], branches)


def solution(mesh):
    return jax.shard_map(
        body,
        mesh=mesh,
        in_specs=(
            P(("grp", "col"), None, None),
            P(),
            P(),
            P(),
            P(("grp", "col"), None, None),
            P(("grp", "col"), None),
        ),
        out_specs=(P("grp", "col", None), P(("grp", "col"), None, None)),
        check_vma=False,
    )
```

```python
import functools

import jax
import jax.numpy as jnp
from jax import lax
from jax.experimental import pallas as pl
from jax.experimental.pallas import tpu as pltpu
from jax.sharding import PartitionSpec as P

MESH = pl.DeviceIdType.MESH
LANES = 128
UNIT = 4096
BAG = 16
ROWS = 32768
CHUNKS = 4
ORDER = ((1, 0), (3, 0), (2, 0), (0, 0), (3, 1), (4, 0), (5, 0), (3, 2), (4, 1), (5, 1), (6, 0), (3, 3), (4, 2), (5, 2), (6, 1), (4, 3), (5, 3), (6, 2), (6, 3))
HOLD = 88
LEVELS = ((60, 27), (64, 29), (72, 31), (88, 32))
LEVELS_ID = len(LEVELS)
LISTS3, SLOTS, COUNTS, INVERSE, MINE, LEVEL = 8, 24, 25, 26, 27, 28


def place(index):
    core = lax.rem(index, 2)
    x = lax.rem(lax.div(index, 2), 4)
    y = lax.rem(lax.div(index, 8), 4)
    z = lax.div(index, 32)
    return y, x, core, z


def peer_of(offset, me):
    dy, dx, dc, dz = place(offset)
    y, x, core, z = me
    ty, tx = lax.rem(y + dy, 4), lax.rem(x + dx, 4)
    tc, tz = lax.rem(core + dc, 2), lax.rem(z + dz, 4)
    return (ty * 4 + tx) * 2 + tc, tz


def greet_all(groups, cols, me):
    barrier = pltpu.get_barrier_semaphore()

    def greet(i, carry):
        to_grp, to_col = peer_of(i, me)
        pl.semaphore_signal(barrier, inc=1, device_id=(to_grp, to_col), device_id_type=MESH)
        return carry

    lax.fori_loop(1, groups * cols, greet, 0)
    return barrier


def load_table(groups, table_ref, blocks, sem):
    def load(j, carry):
        pltpu.make_async_copy(
            table_ref.at[0, :, pl.ds(pl.multiple_of(j * LANES, LANES), LANES)],
            blocks.at[lax.div(j, groups), lax.rem(j, groups)],
            sem,
        ).start()
        return carry

    lax.fori_loop(0, table_ref.shape[2] // LANES, load, 0)


def send_rows(groups, cols, stride, me, own, source, target, send_sem, recv_sem):
    devices = groups * cols

    def send(i, carry):
        to_grp, to_col = peer_of(lax.rem(i * stride, devices), me)
        pltpu.make_async_remote_copy(
            src_ref=source.at[to_grp * cols + to_col],
            dst_ref=target.at[own],
            send_sem=send_sem,
            recv_sem=recv_sem,
            device_id=(to_grp, to_col),
            device_id_type=MESH,
        ).start()
        return carry

    lax.fori_loop(1, devices, send, 0)


def turn_table(groups, blocks, rows_by_id):
    units, _, width, _ = blocks.shape
    table_len = units * groups * LANES

    def turn(j, carry):
        for u in range(4):
            p = lax.rem(j, groups // 4) * 4 + u
            unit = lax.div(j, groups // 4)
            start = pl.multiple_of((unit * groups + p) * LANES, LANES)
            rows_by_id[pl.ds(start, LANES), :] = blocks[unit, p].T.astype(jnp.float32)
        return carry

    lax.fori_loop(0, units * groups // 4, turn, 0)
    rows_by_id[pl.ds(table_len, 8), :] = jnp.zeros((8, width), jnp.float32)


def pool_bags(devices, rows_by_id, ids_in, ids_smem, sums, ids_recv_sem, local_sem):
    wait_for(ids_in.at[pl.ds(0, devices - 1)], ids_recv_sem)
    to_smem = pltpu.make_async_copy(ids_in, ids_smem, local_sem)
    to_smem.start()
    to_smem.wait()
    samples = sums.shape[1]

    def pool(d, carry):
        for b in range(samples):
            terms = [rows_by_id[pl.ds(ids_smem[d, 0, b * BAG + i], 1), :] for i in range(BAG)]
            while len(terms) > 1:
                terms = [terms[k] + terms[k + 1] for k in range(0, len(terms), 2)]
            sums[d, b : b + 1, :] = terms[0]
        return carry

    lax.fori_loop(0, devices, pool, 0)


def wait_for(ref, sem):
    pltpu.make_async_copy(ref, ref, sem).wait()


def exchange_kernel(
    groups, cols, stride, tables_ref, ids_ref, table_ref, out_ref, ret_ref,
    blocks, landed, packed, rows_by_id, ids_in, ids_smem, sums,
    local_sem, send_sem, recv_sem, send2_sem, recv2_sem,
    ids_send_sem, ids_recv_sem, sum_send_sem, sum_recv_sem,
):
    devices = groups * cols
    width = table_ref.shape[1]
    narrow = width // cols
    grp = lax.axis_index("grp")
    col = lax.axis_index("col")
    own = grp * cols + col
    me = (lax.div(grp, 8), lax.rem(lax.div(grp, 2), 4), lax.rem(grp, 2), col)

    barrier = greet_all(groups, cols, me)
    load_table(groups, table_ref, blocks, local_sem)
    pl.semaphore_wait(barrier, devices - 1)
    send_rows(groups, cols, stride, me, own, ids_ref, ids_in, ids_send_sem, ids_recv_sem)
    ids_in[own] = ids_ref[own]
    wait_for(blocks, local_sem)

    def send(i, carry):
        offset = lax.rem(i * stride, devices)
        to_grp, to_col = peer_of(offset, me)
        pltpu.make_async_remote_copy(
            src_ref=blocks.at[:, to_grp, pl.ds(pl.multiple_of(to_col * narrow, narrow), narrow), :],
            dst_ref=landed.at[own],
            send_sem=send_sem,
            recv_sem=recv_sem,
            device_id=(to_grp, to_col),
            device_id_type=MESH,
        ).start()
        return carry

    lax.fori_loop(1, devices, send, 0)
    landed[own] = blocks[:, grp, pl.ds(pl.multiple_of(col * narrow, narrow), narrow), :]

    turn_table(groups, blocks, rows_by_id)
    pool_bags(devices, rows_by_id, ids_in, ids_smem, sums, ids_recv_sem, local_sem)
    send_rows(groups, cols, stride, me, own, sums, ret_ref, sum_send_sem, sum_recv_sem)
    own_sums = pltpu.make_async_copy(sums.at[own], ret_ref.at[own], local_sem)
    own_sums.start()
    own_sums.wait()
    everyone = landed.at[pl.ds(0, devices - 1)]
    wait_for(everyone, recv_sem)

    per_group = packed.shape[1]

    def pack(j, carry):
        slot = tables_ref[SLOTS, j]
        count = tables_ref[COUNTS, j]
        block = landed[slot]
        unit = lax.broadcasted_iota(jnp.int32, block.shape, 0)
        packed[lax.div(j, per_group), lax.rem(j, per_group)] = jnp.where(
            unit < count, block, jnp.zeros_like(block)
        )
        return carry

    lax.fori_loop(0, groups * per_group, pack, 0)

    def send2(i, carry):
        offset = lax.rem(lax.rem(i, groups - 1) + 1, groups) * 27
        q = lax.div(i, groups - 1)
        to_grp, _ = peer_of(lax.rem(offset, groups), me)
        pltpu.make_async_remote_copy(
            src_ref=packed.at[to_grp, q],
            dst_ref=out_ref.at[grp, q],
            send_sem=send2_sem,
            recv_sem=recv2_sem,
            device_id=(to_grp, col),
            device_id_type=MESH,
        ).start()
        return carry

    lax.fori_loop(0, per_group * (groups - 1), send2, 0)
    mine = pltpu.make_async_copy(packed.at[grp], out_ref.at[grp], local_sem)
    mine.start()
    mine.wait()
    wait_for(everyone, send_sem)
    wait_for(packed.at[pl.ds(0, groups - 1)], send2_sem)
    wait_for(out_ref.at[pl.ds(0, groups - 1)], recv2_sem)
    wait_for(ids_in.at[pl.ds(0, devices - 1)], ids_send_sem)
    wait_for(sums.at[pl.ds(0, devices - 1)], sum_send_sem)
    wait_for(ret_ref.at[pl.ds(0, devices - 1)], sum_recv_sem)


def exchange(tables, ids, old_tables, groups, cols, stride=37):
    _, width, table_len = old_tables.shape
    devices = groups * cols
    narrow = width // cols
    per_group = tables.shape[1] // groups
    column_blocks = table_len // LANES
    units = column_blocks // groups
    dtype = old_tables.dtype
    samples = LANES // BAG
    return pl.pallas_call(
        functools.partial(exchange_kernel, groups, cols, stride),
        out_shape=(
            jax.ShapeDtypeStruct((groups, per_group, units, narrow, LANES), dtype),
            jax.ShapeDtypeStruct((devices, samples, width), jnp.float32),
        ),
        in_specs=[
            pl.BlockSpec(memory_space=pltpu.SMEM),
            pl.BlockSpec(memory_space=pltpu.VMEM),
            pl.BlockSpec(memory_space=pl.ANY),
        ],
        out_specs=(pl.BlockSpec(memory_space=pl.ANY), pl.BlockSpec(memory_space=pl.ANY)),
        scratch_shapes=[
            pltpu.VMEM((units, groups, width, LANES), dtype),
            pltpu.VMEM((devices, units, narrow, LANES), dtype),
            pltpu.VMEM((groups, per_group, units, narrow, LANES), dtype),
            pltpu.VMEM((table_len + 8, width), jnp.float32),
            pltpu.VMEM((devices, 1, LANES), jnp.int32),
            pltpu.SMEM((devices, 1, LANES), jnp.int32),
            pltpu.VMEM((devices, samples, width), jnp.float32),
        ]
        + [pltpu.SemaphoreType.DMA] * 9,
        compiler_params=pltpu.CompilerParams(
            collective_id=LEVELS_ID, has_side_effects=True, vmem_limit_bytes=60 * 1024 * 1024
        ),
        name="exchange",
    )(tables, ids, old_tables)


def route_kernel(
    groups, cols, stride, cap2, cap3, hold, chunks,
    tables_ref, ids_ref, table_ref, out_ref, ret_ref,
    blocks, rows_by_id, ids_in, ids_smem, sums, first, outgoing, second, final,
    local_sem, ids_send_sem, ids_recv_sem, sum_send_sem, sum_recv_sem,
    send1_sem, recv1_sem, send2_sem, recv2_sem, send3_sem, recv3_sem, own3_sem,
):
    devices = groups * cols
    width = blocks.shape[2]
    narrow = width // cols
    piece = first[0].shape[1]
    parts = narrow // piece
    grp = lax.axis_index("grp")
    col = lax.axis_index("col")
    own = grp * cols + col
    y, x, core = lax.div(grp, 8), lax.rem(lax.div(grp, 2), 4), lax.rem(grp, 2)
    me = (y, x, core, col)
    along = (y, x)
    across = (x, y)
    line = 8
    source = [(along[h] * 2 + core) * cols + col for h in range(2)]
    seat = [along[h] * 2 + core for h in range(2)]

    def at(h, u, v, c):
        return ((u * 4 + v) * 2 + c) if h == 0 else ((v * 4 + u) * 2 + c)

    barrier = greet_all(groups, cols, me)
    load_table(groups, table_ref, blocks, local_sem)
    pl.semaphore_wait(barrier, devices - 1)
    wait_for(blocks, local_sem)

    def ids_out():
        send_rows(groups, cols, stride, me, own, ids_ref, ids_in, ids_send_sem, ids_recv_sem)
        ids_in[own] = ids_ref[own]

    def turn():
        turn_table(groups, blocks, rows_by_id)

    def stage1(n):
        c, w = n // parts, n % parts

        def send(i, carry):
            o = lax.rem(i * 5, 32)
            dc, du, dz = lax.rem(o, 2), lax.rem(lax.div(o, 2), 4), lax.div(o, 8)
            tz = lax.rem(col + dz, 4)
            tc = lax.rem(core + dc, 2)
            start = pl.multiple_of(tz * narrow + w * piece, piece)
            for h in range(2):
                tu = lax.rem(along[h] + du, 4)
                pltpu.make_async_remote_copy(
                    src_ref=blocks.at[:, h * 16 + c * 8 + tu * 2 + tc, pl.ds(start, piece), :],
                    dst_ref=first[h * chunks + n].at[pl.ds(source[h] * 8, 8)],
                    send_sem=send1_sem.at[h * chunks + n],
                    recv_sem=recv1_sem.at[h * chunks + n],
                    device_id=(at(h, tu, across[h], tc), tz),
                    device_id_type=MESH,
                ).start()
            return carry

        lax.fori_loop(1, 32, send, 0)
        start = pl.multiple_of(col * narrow + w * piece, piece)
        for h in range(2):
            first[h * chunks + n][pl.ds(source[h] * 8, 8)] = blocks[
                :, h * 16 + c * 8 + seat[h], pl.ds(start, piece), :
            ]

    def arrived1(n):
        for h in range(2):
            i = h * chunks + n
            wait_for(first[i].at[pl.ds(0, 31 * 8)], recv1_sem.at[i])

    def stage2(n):
        half = cap2 // 2
        for h in range(2):
            i = h * chunks + n

            def pack(m, carry):
                for dv in range(1, 4):
                    for u in range(4):
                        outgoing[i][(dv - 1) * cap2 + m * 4 + u] = first[i][
                            tables_ref[h * 4 + dv, m * 4 + u]
                        ]
                return carry

            lax.fori_loop(0, cap2 // 4, pack, 0)
            for m in range(2):
                for dv in (1, 3, 2):
                    pltpu.make_async_remote_copy(
                        src_ref=outgoing[i].at[pl.ds((dv - 1) * cap2 + m * half, half)],
                        dst_ref=second[i].at[pl.ds(dv * hold + m * half, half)],
                        send_sem=send2_sem.at[i],
                        recv_sem=recv2_sem.at[i],
                        device_id=(at(h, along[h], lax.rem(across[h] + dv, 4), core), col),
                        device_id_type=MESH,
                    ).start()
        for h in range(2):
            i = h * chunks + n

            def keep(m, carry):
                for u in range(4):
                    second[i][m * 4 + u] = first[i][tables_ref[h * 4, m * 4 + u]]
                return carry

            lax.fori_loop(0, hold // 4, keep, 0)

    def stage3(n):
        for h in range(2):
            i = h * chunks + n
            wait_for(second[i].at[pl.ds(0, 3 * cap2)], recv2_sem.at[i])

            def pack(m, carry):
                for d in range(line):
                    final[i][d, m] = second[i][tables_ref[LISTS3 + h * line + d, m]]
                return carry

            lax.fori_loop(0, cap3, pack, 0)
            for d in (5, 3, 7, 2, 6, 4, 1):
                tu = lax.rem(along[h] + d // 2, 4)
                tc = lax.rem(core + d % 2, 2)
                pltpu.make_async_remote_copy(
                    src_ref=final[i].at[d],
                    dst_ref=out_ref.at[h, n, seat[h]],
                    send_sem=send3_sem.at[i],
                    recv_sem=recv3_sem.at[i],
                    device_id=(at(h, tu, across[h], tc), col),
                    device_id_type=MESH,
                ).start()
            pltpu.make_async_copy(final[i].at[0], out_ref.at[h, n, seat[h]], own3_sem.at[i]).start()

    def bags():
        pool_bags(devices, rows_by_id, ids_in, ids_smem, sums, ids_recv_sem, local_sem)
        send_rows(groups, cols, stride, me, own, sums, ret_ref, sum_send_sem, sum_recv_sem)
        own_sums = pltpu.make_async_copy(sums.at[own], ret_ref.at[own], local_sem)
        own_sums.start()
        own_sums.wait()

    for stage, n in ORDER:
        steps = (bags, ids_out, turn, stage1, arrived1, stage2, stage3)
        steps[stage](*(() if stage < 3 else (n,)))
    for h in range(2):
        for n in range(chunks):
            i = h * chunks + n
            wait_for(first[i].at[pl.ds(0, 31 * 8)], send1_sem.at[i])
            wait_for(outgoing[i], send2_sem.at[i])
            wait_for(final[i].at[pl.ds(0, line - 1)], send3_sem.at[i])
            wait_for(final[i].at[0], own3_sem.at[i])
            wait_for(out_ref.at[h, n, pl.ds(0, line - 1)], recv3_sem.at[i])
    wait_for(ids_in.at[pl.ds(0, devices - 1)], ids_send_sem)
    wait_for(sums.at[pl.ds(0, devices - 1)], sum_send_sem)
    wait_for(ret_ref.at[pl.ds(0, devices - 1)], sum_recv_sem)


def routed(tables, ids, old_tables, groups, cols, cap2, cap3, number, chunks=CHUNKS, stride=37):
    _, width, table_len = old_tables.shape
    devices = groups * cols
    piece = (width // cols) * 2 // chunks
    units = table_len // LANES // groups
    dtype = old_tables.dtype
    samples = LANES // BAG
    smem = pl.BlockSpec(memory_space=pltpu.SMEM)
    hbm = pl.BlockSpec(memory_space=pl.ANY)
    both = 2 * chunks
    dma = pltpu.SemaphoreType.DMA
    return pl.pallas_call(
        functools.partial(route_kernel, groups, cols, stride, cap2, cap3, HOLD, chunks),
        out_shape=(
            jax.ShapeDtypeStruct((2, chunks, 8, cap3, piece, LANES), dtype),
            jax.ShapeDtypeStruct((devices, samples, width), jnp.float32),
        ),
        in_specs=[smem, pl.BlockSpec(memory_space=pltpu.VMEM), hbm],
        out_specs=(hbm, hbm),
        scratch_shapes=[
            pltpu.VMEM((units, groups, width, LANES), dtype),
            pltpu.VMEM((table_len + 8, width), jnp.float32),
            pltpu.VMEM((devices, 1, LANES), jnp.int32),
            pltpu.SMEM((devices, 1, LANES), jnp.int32),
            pltpu.VMEM((devices, samples, width), jnp.float32),
            [pltpu.VMEM((devices // 4 * units, piece, LANES), dtype) for _ in range(both)],
            [pltpu.VMEM((3 * cap2, piece, LANES), dtype) for _ in range(both)],
            [pltpu.VMEM((4 * HOLD, piece, LANES), dtype) for _ in range(both)],
            [pltpu.VMEM((8, cap3, piece, LANES), dtype) for _ in range(both)],
        ]
        + [dma] * 5
        + [dma((both,))] * 7,
        compiler_params=pltpu.CompilerParams(
            collective_id=number, has_side_effects=True, vmem_limit_bytes=63 * 1024 * 1024
        ),
        name="routed",
    )(tables, ids, old_tables)


def plan_kernel(old_ref, new_ref, rows_ref, ids_ref, len_ref, tables_ref, ids_out, turned):
    samples, size = len_ref.shape
    grp = lax.axis_index("grp")
    y, x, core = lax.div(grp, 8), lax.rem(lax.div(grp, 2), 4), lax.rem(grp, 2)
    down = lax.broadcasted_iota(jnp.int32, (size, size), 0)
    lane = lax.broadcasted_iota(jnp.int32, (size, size), 1)
    index = lax.broadcasted_iota(jnp.int32, (1, size), 1)

    def column(row):
        return jnp.broadcast_to(row, (size, size)).T

    def total(mask, value):
        return jnp.sum(jnp.where(mask, value, 0), axis=0, keepdims=True)

    def put(row, value):
        tables_ref[row : row + 1, :] = value

    old_down = column(old_ref[...])
    new = new_ref[...]
    slot = total(old_down == new, down)
    count = total(down == new, column(rows_ref[...] // UNIT))
    put(SLOTS, slot)
    put(COUNTS, count)
    put(INVERSE, total(old_down == lane, down))
    count_down = column(count)
    target_down = down // 4
    base = total((target_down == index // 4) & (down < lane), count_down)
    base_down = column(base)
    slot_down = column(slot)
    core_from, z_from = (slot_down // 4) % 2, slot_down % 4
    core_to = target_down % 2
    sides = []
    for place_down, place in ((slot_down // 4, slot // 4), (target_down, index // 4)):
        sides.append(((place_down // 8, (place_down // 2) % 4), (place // 8, (place // 2) % 4)))
    need0 = need2 = jnp.zeros((1, 1), jnp.int32)
    for h, (u, v) in enumerate(((y, x), (x, y))):
        u_from, v_from = sides[0][0][h], sides[0][0][1 - h]
        u_to, v_to = sides[1][0][h], sides[1][0][1 - h]
        pair_down = v_from * 4 + v_to
        pair = sides[0][1][1 - h] * 4 + sides[1][1][1 - h]
        begun = total((pair_down == pair) & (down < lane), count_down)
        begun_down = column(begun)
        sums = total(pair_down == lane, count_down)
        same = index % 5 == 0
        need0 = jnp.maximum(need0, jnp.max(jnp.where(same, sums, 0), axis=1, keepdims=True))
        need2 = jnp.maximum(need2, jnp.max(jnp.where(same, 0, sums), axis=1, keepdims=True))
        step = (v_to - v_from + 4) % 4
        source = ((u_from * 2 + core_from) * 4 + z_from) * 8 + lane - begun_down
        inside = (v_from == v) & (lane >= begun_down) & (lane < begun_down + count_down)
        for dv in range(4):
            put(h * 4 + dv, total(inside & (step == dv), source))
        rel = ((u_to - u + 4) % 4) * 2 + (core_to - core + 2) % 2
        held = step * HOLD + jnp.minimum(begun_down + lane - base_down, HOLD - 1)
        inside = (v_to == v) & (lane >= base_down) & (lane < base_down + count_down)
        for d in range(8):
            put(LISTS3 + h * 8 + d, total(inside & (rel == d), held))
    need3 = jnp.max(total(target_down == lane, count_down), axis=1, keepdims=True)
    level = jnp.full((1, 1), len(LEVELS), jnp.int32)
    for number in reversed(range(len(LEVELS))):
        cap2, cap3 = LEVELS[number]
        fits = (need0 <= HOLD) & (need2 <= cap2) & (need3 <= cap3)
        level = jnp.where(fits, number, level)
    put(LEVEL, jnp.broadcast_to(level, (1, size)))
    mine = total(down == grp * 4 + lane, count_down)
    offset = total(down == grp * 4 + lane - 4, base_down)
    put(MINE, jnp.where(index < 4, mine, offset))

    turn_in = lax.broadcasted_iota(jnp.int32, (BAG, size), 0)
    parts = []
    for b in range(samples):
        used = turn_in < len_ref[b : b + 1, :]
        parts.append(jnp.where(used, ids_ref[b * BAG : (b + 1) * BAG, :], ROWS))
    flat = jnp.concatenate(parts, axis=0).T
    high = jnp.dot(
        (old_down == lane).astype(jnp.bfloat16), (flat // 256).astype(jnp.bfloat16),
        preferred_element_type=jnp.float32,
    )
    low = jnp.dot(
        (old_down == lane).astype(jnp.bfloat16), (flat % 256).astype(jnp.bfloat16),
        preferred_element_type=jnp.float32,
    )
    turned[...] = high.astype(jnp.int32) * 256 + low.astype(jnp.int32)

    def copy(s, carry):
        for i in range(8):
            ids_out[s * 8 + i] = turned[pl.ds(s * 8 + i, 1), :]
        return carry

    lax.fori_loop(0, size // 8, copy, 0)


def plan(old_plan, new_plan, table_rows, ids, bag_len):
    tables = old_plan.shape[0]
    vmem = pl.BlockSpec(memory_space=pltpu.VMEM)
    flat = jnp.transpose(ids, (0, 2, 1)).reshape(-1, tables)
    return pl.pallas_call(
        plan_kernel,
        out_shape=(
            jax.ShapeDtypeStruct((32, tables), jnp.int32),
            jax.ShapeDtypeStruct((tables, 1, flat.shape[0]), jnp.int32),
        ),
        in_specs=[vmem] * 5,
        out_specs=(vmem, vmem),
        scratch_shapes=[pltpu.VMEM((tables, flat.shape[0]), jnp.int32)],
        name="plan",
    )(old_plan[None], new_plan[None], table_rows[None], flat, bag_len)


def reorder_sums(share, tables_ref, ret_ref, pooled_ref):
    samples = pooled_ref.shape[0]
    first = (pl.program_id(0) * pl.num_programs(1) + pl.program_id(1)) * share

    def reorder(i, carry):
        table = first + i
        rows = ret_ref[tables_ref[INVERSE, table]]
        for b in range(samples):
            pooled_ref[b, pl.ds(table, 1), :] = rows[b : b + 1, :]
        return carry

    lax.fori_loop(0, share, reorder, 0)


def unpack_kernel(steps, tables_ref, in_ref, ret_ref, out_ref, pooled_ref):
    groups, _, units = in_ref.shape[:3]
    for k in range(units):
        for p in range(groups):
            start = (k * groups + p) * LANES
            out_ref[0, :, start : start + LANES] = in_ref[p, 0, k]
    reorder_sums(tables_ref.shape[1] // steps, tables_ref, ret_ref, pooled_ref)


def unpack_routed_kernel(
    tables_ref, in_ref, ret_in_ref, out_ref, pooled_ref, taken, built, ret, in_sem, ret_sem, out_sem
):
    halves, chunks, seats, cap3, piece, lanes = in_ref.shape
    per_group, narrow, table_len = out_ref.shape
    parts = narrow // piece
    units = table_len // UNIT
    tables = ret.shape[0]
    samples = ret.shape[1]
    split = 2
    fetched = pltpu.make_async_copy(ret_in_ref, ret, ret_sem)

    def low(q):
        return jnp.minimum(tables_ref[MINE, 4 + q], cap3 - units)

    for q in range(per_group):
        for h in range(halves):
            for n in range(chunks):
                pltpu.make_async_copy(
                    in_ref.at[h, n, :, pl.ds(low(q), units)], taken.at[q, h, n], in_sem.at[q]
                ).start()
    fetched.start()

    def put_out(q, r):
        size = table_len // split
        return pltpu.make_async_copy(
            built.at[q, :, pl.ds(r * size, size)], out_ref.at[q, :, pl.ds(r * size, size)],
            out_sem.at[q * split + r],
        )

    for q in range(per_group):
        count, base = tables_ref[MINE, q], tables_ref[MINE, 4 + q] - low(q)
        wait_for(taken.at[q], in_sem.at[q])
        for r in range(split):

            def build(k, carry):
                begin = pl.multiple_of(k * UNIT, UNIT)

                @pl.when(k < count)
                def _():
                    for h in range(halves):
                        for n in range(chunks):
                            c, w = n // parts, n % parts
                            for p in range(seats):
                                start = begin + (h * 16 + c * 8 + p) * lanes
                                built[q, w * piece : (w + 1) * piece, pl.ds(start, lanes)] = taken[
                                    q, h, n, p, base + k
                                ]

                @pl.when(k >= count)
                def _():
                    built[q, :, pl.ds(begin, UNIT)] = jnp.zeros((narrow, UNIT), built.dtype)

                return carry

            lax.fori_loop(r * units // split, (r + 1) * units // split, build, 0)
            put_out(q, r).start()
    fetched.wait()

    def reorder(i, carry):
        for u in range(4):
            rows = ret[tables_ref[INVERSE, i * 4 + u]]
            for b in range(samples):
                pooled_ref[b, pl.ds(i * 4 + u, 1), :] = rows[b : b + 1, :]
        return carry

    lax.fori_loop(0, tables // 4, reorder, 0)
    for q in range(per_group):
        for r in range(split):
            put_out(q, r).wait()


def unpack_routed(tables, received, returned, narrow, table_len):
    halves, chunks, seats, _, piece, lanes = received.shape
    devices, samples, width = returned.shape
    hbm = pl.BlockSpec(memory_space=pl.ANY)
    units = table_len // UNIT
    dma = pltpu.SemaphoreType.DMA
    return pl.pallas_call(
        unpack_routed_kernel,
        out_shape=(
            jax.ShapeDtypeStruct((4, narrow, table_len), received.dtype),
            jax.ShapeDtypeStruct((samples, devices, width), returned.dtype),
        ),
        in_specs=[pl.BlockSpec(memory_space=pltpu.SMEM), hbm, hbm],
        out_specs=(hbm, pl.BlockSpec(memory_space=pltpu.VMEM)),
        scratch_shapes=[
            pltpu.VMEM((4, halves, chunks, seats, units, piece, lanes), received.dtype),
            pltpu.VMEM((4, narrow, table_len), received.dtype),
            pltpu.VMEM(returned.shape, returned.dtype),
            dma((4,)),
            dma,
            dma((8,)),
        ],
        compiler_params=pltpu.CompilerParams(vmem_limit_bytes=62 * 1024 * 1024),
        name="unpack_routed",
    )(tables, received, returned)


def unpack(kernel, block, index, tables, received, returned, narrow, table_len, step=4):
    devices, samples, width = returned.shape
    per_group = 4
    splits = table_len // UNIT // step
    smem = pl.BlockSpec(memory_space=pltpu.SMEM)
    return pl.pallas_call(
        functools.partial(kernel, per_group * splits),
        out_shape=(
            jax.ShapeDtypeStruct((per_group, narrow, table_len), received.dtype),
            jax.ShapeDtypeStruct((samples, devices, width), returned.dtype),
        ),
        grid=(per_group, splits),
        in_specs=[
            smem,
            pl.BlockSpec(block, index),
            pl.BlockSpec((devices, samples, width), lambda q, k: (0, 0, 0)),
        ],
        out_specs=(
            pl.BlockSpec((1, narrow, step * UNIT), lambda q, k: (q, 0, k)),
            pl.BlockSpec((samples, devices, width), lambda q, k: (0, 0, 0)),
        ),
        compiler_params=pltpu.CompilerParams(vmem_limit_bytes=40 * 1024 * 1024),
        name="unpack",
    )(tables, received, returned)


def body(old_tables, table_rows, old_plan, new_plan, ids, bag_len):
    groups = lax.axis_size("grp")
    cols = lax.axis_size("col")
    _, width, table_len = old_tables.shape
    narrow = width // cols
    tables, own_ids = plan(old_plan, new_plan, table_rows, ids, bag_len)

    def by_level(number):
        cap2, cap3 = LEVELS[number]

        def run():
            received, returned = routed(
                tables, own_ids, old_tables, groups, cols, cap2, cap3, number
            )
            return unpack_routed(tables, received, returned, narrow, table_len)

        return run

    def spread():
        received, returned = exchange(tables, own_ids, old_tables, groups, cols)
        block = received.shape[:1] + (1, 4) + received.shape[3:]
        return unpack(
            unpack_kernel, block, lambda q, k: (0, q, k, 0, 0),
            tables, received, returned, narrow, table_len,
        )

    branches = [by_level(number) for number in range(len(LEVELS))] + [spread]
    return lax.switch(tables[LEVEL, 0], branches)


def solution(mesh):
    return jax.shard_map(
        body,
        mesh=mesh,
        in_specs=(
            P(("grp", "col"), None, None),
            P(),
            P(),
            P(),
            P(("grp", "col"), None, None),
            P(("grp", "col"), None),
        ),
        out_specs=(P("grp", "col", None), P(("grp", "col"), None, None)),
        check_vma=False,
    )
```

```python
import functools

import jax
import jax.numpy as jnp
from jax import lax
from jax.experimental import pallas as pl
from jax.experimental.pallas import tpu as pltpu
from jax.sharding import PartitionSpec as P

MESH = pl.DeviceIdType.MESH
LANES = 128
UNIT = 4096
BAG = 16
ROWS = 32768
CHUNKS = 4
ORDER = ((1, 2), (4, 0), (2, 2), (4, 1), (0, 2), (3, 2), (5, 0), (6, 0), (4, 3), (5, 1), (6, 1), (4, 4), (5, 3), (6, 3), (7, 0), (4, 6), (5, 4), (6, 4), (7, 1), (4, 7), (5, 6), (6, 6), (7, 3), (4, 9), (5, 7), (6, 7), (7, 4), (4, 10), (5, 9), (6, 9), (7, 6), (5, 10), (6, 10), (7, 7), (7, 9), (7, 10))
HOLD = 88
LEVELS = ((60, 27), (64, 29), (72, 31), (88, 32))
LEVELS_ID = len(LEVELS)
LISTS3, SLOTS, COUNTS, INVERSE, MINE = 8, 24, 25, 26, 27


def place(index):
    core = lax.rem(index, 2)
    x = lax.rem(lax.div(index, 2), 4)
    y = lax.rem(lax.div(index, 8), 4)
    z = lax.div(index, 32)
    return y, x, core, z


def peer_of(offset, me):
    dy, dx, dc, dz = place(offset)
    y, x, core, z = me
    ty, tx = lax.rem(y + dy, 4), lax.rem(x + dx, 4)
    tc, tz = lax.rem(core + dc, 2), lax.rem(z + dz, 4)
    return (ty * 4 + tx) * 2 + tc, tz


def greet_all(groups, cols, me):
    barrier = pltpu.get_barrier_semaphore()

    def greet(i, carry):
        to_grp, to_col = peer_of(i, me)
        pl.semaphore_signal(barrier, inc=1, device_id=(to_grp, to_col), device_id_type=MESH)
        return carry

    lax.fori_loop(1, groups * cols, greet, 0)
    return barrier


def load_table(groups, table_ref, blocks, sem):
    def load(j, carry):
        pltpu.make_async_copy(
            table_ref.at[0, :, pl.ds(pl.multiple_of(j * LANES, LANES), LANES)],
            blocks.at[lax.div(j, groups), lax.rem(j, groups)],
            sem,
        ).start()
        return carry

    lax.fori_loop(0, table_ref.shape[2] // LANES, load, 0)


def send_rows(groups, cols, stride, me, own, source, target, send_sem, recv_sem):
    devices = groups * cols

    def send(i, carry):
        to_grp, to_col = peer_of(lax.rem(i * stride, devices), me)
        pltpu.make_async_remote_copy(
            src_ref=source.at[to_grp * cols + to_col],
            dst_ref=target.at[own],
            send_sem=send_sem,
            recv_sem=recv_sem,
            device_id=(to_grp, to_col),
            device_id_type=MESH,
        ).start()
        return carry

    lax.fori_loop(1, devices, send, 0)


def turn_table(groups, blocks, rows_by_id):
    units, _, width, _ = blocks.shape
    table_len = units * groups * LANES

    def turn(j, carry):
        for u in range(4):
            p = lax.rem(j, groups // 4) * 4 + u
            unit = lax.div(j, groups // 4)
            start = pl.multiple_of((unit * groups + p) * LANES, LANES)
            rows_by_id[pl.ds(start, LANES), :] = blocks[unit, p].T.astype(jnp.float32)
        return carry

    lax.fori_loop(0, units * groups // 4, turn, 0)
    rows_by_id[pl.ds(table_len, 8), :] = jnp.zeros((8, width), jnp.float32)


def pool_bags(devices, rows_by_id, ids_in, ids_smem, sums, ids_recv_sem, local_sem):
    wait_for(ids_in.at[pl.ds(0, devices - 1)], ids_recv_sem)
    to_smem = pltpu.make_async_copy(ids_in, ids_smem, local_sem)
    to_smem.start()
    to_smem.wait()
    samples = sums.shape[1]

    def pool(d, carry):
        for b in range(samples):
            terms = [rows_by_id[pl.ds(ids_smem[d, 0, b * BAG + i], 1), :] for i in range(BAG)]
            while len(terms) > 1:
                terms = [terms[k] + terms[k + 1] for k in range(0, len(terms), 2)]
            sums[d, b : b + 1, :] = terms[0]
        return carry

    lax.fori_loop(0, devices, pool, 0)


def wait_for(ref, sem):
    pltpu.make_async_copy(ref, ref, sem).wait()


def exchange_kernel(
    groups, cols, stride, tables_ref, ids_ref, table_ref, out_ref, ret_ref,
    blocks, landed, packed, rows_by_id, ids_in, ids_smem, sums,
    local_sem, send_sem, recv_sem, send2_sem, recv2_sem,
    ids_send_sem, ids_recv_sem, sum_send_sem, sum_recv_sem,
):
    devices = groups * cols
    width = table_ref.shape[1]
    narrow = width // cols
    grp = lax.axis_index("grp")
    col = lax.axis_index("col")
    own = grp * cols + col
    me = (lax.div(grp, 8), lax.rem(lax.div(grp, 2), 4), lax.rem(grp, 2), col)

    barrier = greet_all(groups, cols, me)
    load_table(groups, table_ref, blocks, local_sem)
    pl.semaphore_wait(barrier, devices - 1)
    send_rows(groups, cols, stride, me, own, ids_ref, ids_in, ids_send_sem, ids_recv_sem)
    ids_in[own] = ids_ref[own]
    wait_for(blocks, local_sem)

    def send(i, carry):
        offset = lax.rem(i * stride, devices)
        to_grp, to_col = peer_of(offset, me)
        pltpu.make_async_remote_copy(
            src_ref=blocks.at[:, to_grp, pl.ds(pl.multiple_of(to_col * narrow, narrow), narrow), :],
            dst_ref=landed.at[own],
            send_sem=send_sem,
            recv_sem=recv_sem,
            device_id=(to_grp, to_col),
            device_id_type=MESH,
        ).start()
        return carry

    lax.fori_loop(1, devices, send, 0)
    landed[own] = blocks[:, grp, pl.ds(pl.multiple_of(col * narrow, narrow), narrow), :]

    turn_table(groups, blocks, rows_by_id)
    pool_bags(devices, rows_by_id, ids_in, ids_smem, sums, ids_recv_sem, local_sem)
    send_rows(groups, cols, stride, me, own, sums, ret_ref, sum_send_sem, sum_recv_sem)
    own_sums = pltpu.make_async_copy(sums.at[own], ret_ref.at[own], local_sem)
    own_sums.start()
    own_sums.wait()
    everyone = landed.at[pl.ds(0, devices - 1)]
    wait_for(everyone, recv_sem)

    per_group = packed.shape[1]

    def pack(j, carry):
        slot = tables_ref[SLOTS, j]
        count = tables_ref[COUNTS, j]
        block = landed[slot]
        unit = lax.broadcasted_iota(jnp.int32, block.shape, 0)
        packed[lax.div(j, per_group), lax.rem(j, per_group)] = jnp.where(
            unit < count, block, jnp.zeros_like(block)
        )
        return carry

    lax.fori_loop(0, groups * per_group, pack, 0)

    def send2(i, carry):
        offset = lax.rem(lax.rem(i, groups - 1) + 1, groups) * 27
        q = lax.div(i, groups - 1)
        to_grp, _ = peer_of(lax.rem(offset, groups), me)
        pltpu.make_async_remote_copy(
            src_ref=packed.at[to_grp, q],
            dst_ref=out_ref.at[grp, q],
            send_sem=send2_sem,
            recv_sem=recv2_sem,
            device_id=(to_grp, col),
            device_id_type=MESH,
        ).start()
        return carry

    lax.fori_loop(0, per_group * (groups - 1), send2, 0)
    mine = pltpu.make_async_copy(packed.at[grp], out_ref.at[grp], local_sem)
    mine.start()
    mine.wait()
    wait_for(everyone, send_sem)
    wait_for(packed.at[pl.ds(0, groups - 1)], send2_sem)
    wait_for(out_ref.at[pl.ds(0, groups - 1)], recv2_sem)
    wait_for(ids_in.at[pl.ds(0, devices - 1)], ids_send_sem)
    wait_for(sums.at[pl.ds(0, devices - 1)], sum_send_sem)
    wait_for(ret_ref.at[pl.ds(0, devices - 1)], sum_recv_sem)


def exchange(tables, ids, old_tables, groups, cols, stride=37):
    _, width, table_len = old_tables.shape
    devices = groups * cols
    narrow = width // cols
    per_group = tables.shape[1] // groups
    column_blocks = table_len // LANES
    units = column_blocks // groups
    dtype = old_tables.dtype
    samples = LANES // BAG
    return pl.pallas_call(
        functools.partial(exchange_kernel, groups, cols, stride),
        out_shape=(
            jax.ShapeDtypeStruct((groups, per_group, units, narrow, LANES), dtype),
            jax.ShapeDtypeStruct((devices, samples, width), jnp.float32),
        ),
        in_specs=[
            pl.BlockSpec(memory_space=pltpu.SMEM),
            pl.BlockSpec(memory_space=pltpu.VMEM),
            pl.BlockSpec(memory_space=pl.ANY),
        ],
        out_specs=(pl.BlockSpec(memory_space=pl.ANY), pl.BlockSpec(memory_space=pl.ANY)),
        scratch_shapes=[
            pltpu.VMEM((units, groups, width, LANES), dtype),
            pltpu.VMEM((devices, units, narrow, LANES), dtype),
            pltpu.VMEM((groups, per_group, units, narrow, LANES), dtype),
            pltpu.VMEM((table_len + 8, width), jnp.float32),
            pltpu.VMEM((devices, 1, LANES), jnp.int32),
            pltpu.SMEM((devices, 1, LANES), jnp.int32),
            pltpu.VMEM((devices, samples, width), jnp.float32),
        ]
        + [pltpu.SemaphoreType.DMA] * 9,
        compiler_params=pltpu.CompilerParams(
            collective_id=LEVELS_ID, has_side_effects=True, vmem_limit_bytes=60 * 1024 * 1024
        ),
        name="exchange",
    )(tables, ids, old_tables)


def route_kernel(
    groups, cols, stride, cap2, cap3, hold, chunks,
    tables_ref, ids_ref, table_ref, out_ref, ret_ref,
    blocks, rows_by_id, ids_in, ids_smem, sums, first, outgoing, second, final,
    local_sem, ids_send_sem, ids_recv_sem, sum_send_sem, sum_recv_sem,
    send1_sem, recv1_sem, send2_sem, recv2_sem, send3_sem, recv3_sem, own3_sem,
):
    devices = groups * cols
    width = blocks.shape[2]
    narrow = width // cols
    piece = first[0].shape[1]
    parts = narrow // piece
    grp = lax.axis_index("grp")
    col = lax.axis_index("col")
    own = grp * cols + col
    y, x, core = lax.div(grp, 8), lax.rem(lax.div(grp, 2), 4), lax.rem(grp, 2)
    me = (y, x, core, col)
    along = (y, x)
    across = (x, y)
    line = 8
    source = [(along[h] * 2 + core) * cols + col for h in range(2)]
    seat = [along[h] * 2 + core for h in range(2)]

    def at(h, u, v, c):
        return ((u * 4 + v) * 2 + c) if h == 0 else ((v * 4 + u) * 2 + c)

    barrier = greet_all(groups, cols, me)
    load_table(groups, table_ref, blocks, local_sem)
    pl.semaphore_wait(barrier, devices - 1)
    wait_for(blocks, local_sem)

    def ids_out():
        send_rows(groups, cols, stride, me, own, ids_ref, ids_in, ids_send_sem, ids_recv_sem)
        ids_in[own] = ids_ref[own]

    def turn():
        turn_table(groups, blocks, rows_by_id)

    def stage1(n, sides=(0, 1)):
        c, w = n // parts, n % parts

        def send(i, carry):
            o = lax.rem(i * 5, 32)
            dc, du, dz = lax.rem(o, 2), lax.rem(lax.div(o, 2), 4), lax.div(o, 8)
            tz = lax.rem(col + dz, 4)
            tc = lax.rem(core + dc, 2)
            start = pl.multiple_of(tz * narrow + w * piece, piece)
            for h in sides:
                tu = lax.rem(along[h] + du, 4)
                pltpu.make_async_remote_copy(
                    src_ref=blocks.at[:, h * 16 + c * 8 + tu * 2 + tc, pl.ds(start, piece), :],
                    dst_ref=first[h * chunks + n].at[pl.ds(source[h] * 8, 8)],
                    send_sem=send1_sem.at[h * chunks + n],
                    recv_sem=recv1_sem.at[h * chunks + n],
                    device_id=(at(h, tu, across[h], tc), tz),
                    device_id_type=MESH,
                ).start()
            return carry

        lax.fori_loop(1, 32, send, 0)
        start = pl.multiple_of(col * narrow + w * piece, piece)
        for h in sides:
            first[h * chunks + n][pl.ds(source[h] * 8, 8)] = blocks[
                :, h * 16 + c * 8 + seat[h], pl.ds(start, piece), :
            ]

    def arrived1(n, sides=(0, 1)):
        for h in sides:
            i = h * chunks + n
            wait_for(first[i].at[pl.ds(0, 31 * 8)], recv1_sem.at[i])

    def stage2(n, sides=(0, 1)):
        half = cap2 // 2
        for h in sides:
            i = h * chunks + n

            def pack(m, carry):
                for dv in range(1, 4):
                    for u in range(4):
                        outgoing[i][(dv - 1) * cap2 + m * 4 + u] = first[i][
                            tables_ref[h * 4 + dv, m * 4 + u]
                        ]
                return carry

            lax.fori_loop(0, cap2 // 4, pack, 0)
            for m in range(2):
                for dv in (1, 3, 2):
                    pltpu.make_async_remote_copy(
                        src_ref=outgoing[i].at[pl.ds((dv - 1) * cap2 + m * half, half)],
                        dst_ref=second[i].at[pl.ds(dv * hold + m * half, half)],
                        send_sem=send2_sem.at[i],
                        recv_sem=recv2_sem.at[i],
                        device_id=(at(h, along[h], lax.rem(across[h] + dv, 4), core), col),
                        device_id_type=MESH,
                    ).start()
        for h in sides:
            i = h * chunks + n

            def keep(m, carry):
                for u in range(4):
                    second[i][m * 4 + u] = first[i][tables_ref[h * 4, m * 4 + u]]
                return carry

            lax.fori_loop(0, hold // 4, keep, 0)

    def stage3(n, sides=(0, 1)):
        for h in sides:
            i = h * chunks + n
            wait_for(second[i].at[pl.ds(0, 3 * cap2)], recv2_sem.at[i])

            def pack(m, carry):
                for d in range(line):
                    final[i][d, m] = second[i][tables_ref[LISTS3 + h * line + d, m]]
                return carry

            lax.fori_loop(0, cap3, pack, 0)
            for d in (5, 3, 7, 2, 6, 4, 1):
                tu = lax.rem(along[h] + d // 2, 4)
                tc = lax.rem(core + d % 2, 2)
                pltpu.make_async_remote_copy(
                    src_ref=final[i].at[d],
                    dst_ref=out_ref.at[h, n, seat[h]],
                    send_sem=send3_sem.at[i],
                    recv_sem=recv3_sem.at[i],
                    device_id=(at(h, tu, across[h], tc), col),
                    device_id_type=MESH,
                ).start()
            pltpu.make_async_copy(final[i].at[0], out_ref.at[h, n, seat[h]], own3_sem.at[i]).start()

    def bags():
        pool_bags(devices, rows_by_id, ids_in, ids_smem, sums, ids_recv_sem, local_sem)

    def sums_out():
        send_rows(groups, cols, stride, me, own, sums, ret_ref, sum_send_sem, sum_recv_sem)
        pltpu.make_async_copy(sums.at[own], ret_ref.at[own], local_sem).start()

    for stage, n in ORDER:
        steps = (
            bags, ids_out, turn, sums_out, stage1, arrived1, stage2, stage3,
        )
        steps[stage](*(() if stage < 4 else (n // 3, ((0,), (1,), (0, 1))[n % 3])))
    for h in range(2):
        for n in range(chunks):
            i = h * chunks + n
            wait_for(first[i].at[pl.ds(0, 31 * 8)], send1_sem.at[i])
            wait_for(outgoing[i], send2_sem.at[i])
            wait_for(final[i].at[pl.ds(0, line - 1)], send3_sem.at[i])
            wait_for(final[i].at[0], own3_sem.at[i])
            wait_for(out_ref.at[h, n, pl.ds(0, line - 1)], recv3_sem.at[i])
    wait_for(sums.at[own], local_sem)
    wait_for(ids_in.at[pl.ds(0, devices - 1)], ids_send_sem)
    wait_for(sums.at[pl.ds(0, devices - 1)], sum_send_sem)
    wait_for(ret_ref.at[pl.ds(0, devices - 1)], sum_recv_sem)


def routed(tables, ids, old_tables, groups, cols, cap2, cap3, number, chunks=CHUNKS, stride=37):
    _, width, table_len = old_tables.shape
    devices = groups * cols
    piece = (width // cols) * 2 // chunks
    units = table_len // LANES // groups
    dtype = old_tables.dtype
    samples = LANES // BAG
    smem = pl.BlockSpec(memory_space=pltpu.SMEM)
    hbm = pl.BlockSpec(memory_space=pl.ANY)
    both = 2 * chunks
    dma = pltpu.SemaphoreType.DMA
    return pl.pallas_call(
        functools.partial(route_kernel, groups, cols, stride, cap2, cap3, HOLD, chunks),
        out_shape=(
            jax.ShapeDtypeStruct((2, chunks, 8, cap3, piece, LANES), dtype),
            jax.ShapeDtypeStruct((devices, samples, width), jnp.float32),
        ),
        in_specs=[smem, pl.BlockSpec(memory_space=pltpu.VMEM), hbm],
        out_specs=(hbm, hbm),
        scratch_shapes=[
            pltpu.VMEM((units, groups, width, LANES), dtype),
            pltpu.VMEM((table_len + 8, width), jnp.float32),
            pltpu.VMEM((devices, 1, LANES), jnp.int32),
            pltpu.SMEM((devices, 1, LANES), jnp.int32),
            pltpu.VMEM((devices, samples, width), jnp.float32),
            [pltpu.VMEM((devices // 4 * units, piece, LANES), dtype) for _ in range(both)],
            [pltpu.VMEM((3 * cap2, piece, LANES), dtype) for _ in range(both)],
            [pltpu.VMEM((4 * HOLD, piece, LANES), dtype) for _ in range(both)],
            [pltpu.VMEM((8, cap3, piece, LANES), dtype) for _ in range(both)],
        ]
        + [dma] * 5
        + [dma((both,))] * 7,
        compiler_params=pltpu.CompilerParams(
            collective_id=number, has_side_effects=True, vmem_limit_bytes=63 * 1024 * 1024
        ),
        name="routed",
    )(tables, ids, old_tables)


def plan_kernel(
    old_ref, new_ref, rows_ref, ids_ref, len_ref, tables_ref, level_ref, ids_out, turned
):
    samples, size = len_ref.shape
    grp = lax.axis_index("grp")
    y, x, core = lax.div(grp, 8), lax.rem(lax.div(grp, 2), 4), lax.rem(grp, 2)
    down = lax.broadcasted_iota(jnp.int32, (size, size), 0)
    lane = lax.broadcasted_iota(jnp.int32, (size, size), 1)
    index = lax.broadcasted_iota(jnp.int32, (1, size), 1)

    def column(row):
        return jnp.broadcast_to(row, (size, size)).T

    def total(mask, value):
        return jnp.sum(jnp.where(mask, value, 0), axis=0, keepdims=True)

    def put(row, value):
        tables_ref[row : row + 1, :] = value

    old_down = column(old_ref[...])
    new = new_ref[...]
    slot = total(old_down == new, down)
    count = total(down == new, column(rows_ref[...] // UNIT))
    put(SLOTS, slot)
    put(COUNTS, count)
    put(INVERSE, total(old_down == lane, down))
    count_down = column(count)
    target_down = down // 4
    base = total((target_down == index // 4) & (down < lane), count_down)
    base_down = column(base)
    slot_down = column(slot)
    core_from, z_from = (slot_down // 4) % 2, slot_down % 4
    core_to = target_down % 2
    sides = []
    for place_down, place in ((slot_down // 4, slot // 4), (target_down, index // 4)):
        sides.append(((place_down // 8, (place_down // 2) % 4), (place // 8, (place // 2) % 4)))
    need0 = need2 = jnp.zeros((1, 1), jnp.int32)
    for h, (u, v) in enumerate(((y, x), (x, y))):
        u_from, v_from = sides[0][0][h], sides[0][0][1 - h]
        u_to, v_to = sides[1][0][h], sides[1][0][1 - h]
        pair_down = v_from * 4 + v_to
        pair = sides[0][1][1 - h] * 4 + sides[1][1][1 - h]
        begun = total((pair_down == pair) & (down < lane), count_down)
        begun_down = column(begun)
        sums = total(pair_down == lane, count_down)
        same = index % 5 == 0
        need0 = jnp.maximum(need0, jnp.max(jnp.where(same, sums, 0), axis=1, keepdims=True))
        need2 = jnp.maximum(need2, jnp.max(jnp.where(same, 0, sums), axis=1, keepdims=True))
        step = (v_to - v_from + 4) % 4
        source = ((u_from * 2 + core_from) * 4 + z_from) * 8 + lane - begun_down
        inside = (v_from == v) & (lane >= begun_down) & (lane < begun_down + count_down)
        for dv in range(4):
            put(h * 4 + dv, total(inside & (step == dv), source))
        rel = ((u_to - u + 4) % 4) * 2 + (core_to - core + 2) % 2
        held = step * HOLD + jnp.minimum(begun_down + lane - base_down, HOLD - 1)
        inside = (v_to == v) & (lane >= base_down) & (lane < base_down + count_down)
        for d in range(8):
            put(LISTS3 + h * 8 + d, total(inside & (rel == d), held))
    need3 = jnp.max(total(target_down == lane, count_down), axis=1, keepdims=True)
    level = jnp.full((1, 1), len(LEVELS), jnp.int32)
    for number in reversed(range(len(LEVELS))):
        cap2, cap3 = LEVELS[number]
        fits = (need0 <= HOLD) & (need2 <= cap2) & (need3 <= cap3)
        level = jnp.where(fits, number, level)
    level_ref[0] = level[0, 0]
    mine = total(down == grp * 4 + lane, count_down)
    offset = total(down == grp * 4 + lane - 4, base_down)
    put(MINE, jnp.where(index < 4, mine, offset))

    turn_in = lax.broadcasted_iota(jnp.int32, (BAG, size), 0)
    parts = []
    for b in range(samples):
        used = turn_in < len_ref[b : b + 1, :]
        parts.append(jnp.where(used, ids_ref[b * BAG : (b + 1) * BAG, :], ROWS))
    flat = jnp.concatenate(parts, axis=0).T
    high = jnp.dot(
        (old_down == lane).astype(jnp.bfloat16), (flat // 256).astype(jnp.bfloat16),
        preferred_element_type=jnp.float32,
    )
    low = jnp.dot(
        (old_down == lane).astype(jnp.bfloat16), (flat % 256).astype(jnp.bfloat16),
        preferred_element_type=jnp.float32,
    )
    turned[...] = high.astype(jnp.int32) * 256 + low.astype(jnp.int32)

    def copy(s, carry):
        for i in range(8):
            ids_out[s * 8 + i] = turned[pl.ds(s * 8 + i, 1), :]
        return carry

    lax.fori_loop(0, size // 8, copy, 0)


def plan(old_plan, new_plan, table_rows, ids, bag_len):
    tables = old_plan.shape[0]
    vmem = pl.BlockSpec(memory_space=pltpu.VMEM)
    flat = jnp.transpose(ids, (0, 2, 1)).reshape(-1, tables)
    return pl.pallas_call(
        plan_kernel,
        out_shape=(
            jax.ShapeDtypeStruct((32, tables), jnp.int32),
            jax.ShapeDtypeStruct((1,), jnp.int32),
            jax.ShapeDtypeStruct((tables, 1, flat.shape[0]), jnp.int32),
        ),
        in_specs=[vmem] * 5,
        out_specs=(vmem, pl.BlockSpec(memory_space=pltpu.SMEM), vmem),
        scratch_shapes=[pltpu.VMEM((tables, flat.shape[0]), jnp.int32)],
        name="plan",
    )(old_plan[None], new_plan[None], table_rows[None], flat, bag_len)


def reorder_sums(share, tables_ref, ret_ref, pooled_ref):
    samples = pooled_ref.shape[0]
    first = (pl.program_id(0) * pl.num_programs(1) + pl.program_id(1)) * share

    def reorder(i, carry):
        table = first + i
        rows = ret_ref[tables_ref[INVERSE, table]]
        for b in range(samples):
            pooled_ref[b, pl.ds(table, 1), :] = rows[b : b + 1, :]
        return carry

    lax.fori_loop(0, share, reorder, 0)


def unpack_kernel(steps, tables_ref, in_ref, ret_ref, out_ref, pooled_ref):
    groups, _, units = in_ref.shape[:3]
    for k in range(units):
        for p in range(groups):
            start = (k * groups + p) * LANES
            out_ref[0, :, start : start + LANES] = in_ref[p, 0, k]
    reorder_sums(tables_ref.shape[1] // steps, tables_ref, ret_ref, pooled_ref)


def unpack_routed_kernel(
    tables_ref, in_ref, ret_in_ref, out_ref, pooled_ref, taken, built, ret, in_sem, ret_sem, out_sem
):
    halves, chunks, seats, cap3, piece, lanes = in_ref.shape
    per_group, narrow, table_len = out_ref.shape
    parts = narrow // piece
    units = table_len // UNIT
    tables = ret.shape[0]
    samples = ret.shape[1]
    split = 2
    fetched = pltpu.make_async_copy(ret_in_ref, ret, ret_sem)

    def take(q, k):
        where = jnp.minimum(tables_ref[MINE, 4 + q] + k, cap3 - 1)
        return pltpu.make_async_copy(in_ref.at[:, :, :, where], taken.at[q, k], in_sem.at[q, k])

    for q in range(per_group):

        def ask(k, carry):
            @pl.when(k < tables_ref[MINE, q])
            def _():
                take(q, k).start()

            return carry

        lax.fori_loop(0, units, ask, 0)
    fetched.start()

    def put_out(q, r):
        size = table_len // split
        return pltpu.make_async_copy(
            built.at[q, :, pl.ds(r * size, size)], out_ref.at[q, :, pl.ds(r * size, size)],
            out_sem.at[q * split + r],
        )

    for q in range(per_group):
        count = tables_ref[MINE, q]
        for r in range(split):

            def build(k, carry):
                begin = pl.multiple_of(k * UNIT, UNIT)

                @pl.when(k < count)
                def _():
                    take(q, k).wait()
                    for h in range(halves):
                        for n in range(chunks):
                            c, w = n // parts, n % parts
                            for p in range(seats):
                                start = begin + (h * 16 + c * 8 + p) * lanes
                                built[q, w * piece : (w + 1) * piece, pl.ds(start, lanes)] = taken[
                                    q, k, h, n, p
                                ]

                @pl.when(k >= count)
                def _():
                    built[q, :, pl.ds(begin, UNIT)] = jnp.zeros((narrow, UNIT), built.dtype)

                return carry

            lax.fori_loop(r * units // split, (r + 1) * units // split, build, 0)
            put_out(q, r).start()
    fetched.wait()

    def reorder(i, carry):
        for u in range(4):
            rows = ret[tables_ref[INVERSE, i * 4 + u]]
            for b in range(samples):
                pooled_ref[b, pl.ds(i * 4 + u, 1), :] = rows[b : b + 1, :]
        return carry

    lax.fori_loop(0, tables // 4, reorder, 0)
    for q in range(per_group):
        for r in range(split):
            put_out(q, r).wait()


def unpack_routed(tables, received, returned, narrow, table_len):
    halves, chunks, seats, _, piece, lanes = received.shape
    devices, samples, width = returned.shape
    hbm = pl.BlockSpec(memory_space=pl.ANY)
    units = table_len // UNIT
    dma = pltpu.SemaphoreType.DMA
    return pl.pallas_call(
        unpack_routed_kernel,
        out_shape=(
            jax.ShapeDtypeStruct((4, narrow, table_len), received.dtype),
            jax.ShapeDtypeStruct((samples, devices, width), returned.dtype),
        ),
        in_specs=[pl.BlockSpec(memory_space=pltpu.SMEM), hbm, hbm],
        out_specs=(hbm, pl.BlockSpec(memory_space=pltpu.VMEM)),
        scratch_shapes=[
            pltpu.VMEM((4, units, halves, chunks, seats, piece, lanes), received.dtype),
            pltpu.VMEM((4, narrow, table_len), received.dtype),
            pltpu.VMEM(returned.shape, returned.dtype),
            dma((4, units)),
            dma,
            dma((8,)),
        ],
        compiler_params=pltpu.CompilerParams(vmem_limit_bytes=62 * 1024 * 1024),
        name="unpack_routed",
    )(tables, received, returned)


def unpack(kernel, block, index, tables, received, returned, narrow, table_len, step=4):
    devices, samples, width = returned.shape
    per_group = 4
    splits = table_len // UNIT // step
    smem = pl.BlockSpec(memory_space=pltpu.SMEM)
    return pl.pallas_call(
        functools.partial(kernel, per_group * splits),
        out_shape=(
            jax.ShapeDtypeStruct((per_group, narrow, table_len), received.dtype),
            jax.ShapeDtypeStruct((samples, devices, width), returned.dtype),
        ),
        grid=(per_group, splits),
        in_specs=[
            smem,
            pl.BlockSpec(block, index),
            pl.BlockSpec((devices, samples, width), lambda q, k: (0, 0, 0)),
        ],
        out_specs=(
            pl.BlockSpec((1, narrow, step * UNIT), lambda q, k: (q, 0, k)),
            pl.BlockSpec((samples, devices, width), lambda q, k: (0, 0, 0)),
        ),
        compiler_params=pltpu.CompilerParams(vmem_limit_bytes=40 * 1024 * 1024),
        name="unpack",
    )(tables, received, returned)


def body(old_tables, table_rows, old_plan, new_plan, ids, bag_len):
    groups = lax.axis_size("grp")
    cols = lax.axis_size("col")
    _, width, table_len = old_tables.shape
    narrow = width // cols
    tables, level, own_ids = plan(old_plan, new_plan, table_rows, ids, bag_len)

    def by_level(number):
        cap2, cap3 = LEVELS[number]

        def run():
            received, returned = routed(
                tables, own_ids, old_tables, groups, cols, cap2, cap3, number
            )
            return unpack_routed(tables, received, returned, narrow, table_len)

        return run

    def spread():
        received, returned = exchange(tables, own_ids, old_tables, groups, cols)
        block = received.shape[:1] + (1, 4) + received.shape[3:]
        return unpack(
            unpack_kernel, block, lambda q, k: (0, q, k, 0, 0),
            tables, received, returned, narrow, table_len,
        )

    branches = [by_level(number) for number in range(len(LEVELS))] + [spread]
    return lax.switch(level.reshape(()), branches)


def solution(mesh):
    return jax.shard_map(
        body,
        mesh=mesh,
        in_specs=(
            P(("grp", "col"), None, None),
            P(),
            P(),
            P(),
            P(("grp", "col"), None, None),
            P(("grp", "col"), None),
        ),
        out_specs=(P("grp", "col", None), P(("grp", "col"), None, None)),
        check_vma=False,
    )
```

```python
import functools

import jax
import jax.numpy as jnp
from jax import lax
from jax.experimental import pallas as pl
from jax.experimental.pallas import tpu as pltpu
from jax.sharding import PartitionSpec as P

MESH = pl.DeviceIdType.MESH
LANES = 128
UNIT = 4096
BAG = 16
ROWS = 32768
CHUNKS = 4
ORDER = ((1, 2), (4, 0), (2, 2), (4, 1), (0, 2), (3, 2), (5, 0), (6, 0), (4, 3), (5, 1), (6, 1), (4, 4), (5, 3), (6, 3), (7, 0), (4, 6), (5, 4), (6, 4), (7, 1), (4, 7), (5, 6), (6, 6), (7, 3), (4, 9), (5, 7), (6, 7), (7, 4), (4, 10), (5, 9), (6, 9), (7, 6), (5, 10), (6, 10), (7, 7), (7, 9), (7, 10))
HOLD = 88
LEVELS = ((60, 27), (64, 29), (72, 31), (88, 32))
LEVELS_ID = len(LEVELS)
LISTS3, SLOTS, COUNTS, INVERSE, MINE = 8, 24, 25, 26, 27


def place(index):
    core = lax.rem(index, 2)
    x = lax.rem(lax.div(index, 2), 4)
    y = lax.rem(lax.div(index, 8), 4)
    z = lax.div(index, 32)
    return y, x, core, z


def peer_of(offset, me):
    dy, dx, dc, dz = place(offset)
    y, x, core, z = me
    ty, tx = lax.rem(y + dy, 4), lax.rem(x + dx, 4)
    tc, tz = lax.rem(core + dc, 2), lax.rem(z + dz, 4)
    return (ty * 4 + tx) * 2 + tc, tz


def greet_all(groups, cols, me):
    barrier = pltpu.get_barrier_semaphore()

    def greet(i, carry):
        to_grp, to_col = peer_of(i, me)
        pl.semaphore_signal(barrier, inc=1, device_id=(to_grp, to_col), device_id_type=MESH)
        return carry

    lax.fori_loop(1, groups * cols, greet, 0)
    return barrier


def load_table(groups, table_ref, blocks, sems):
    share = groups // len(sems)
    for k, sem in enumerate(sems):

        def load(j, carry):
            unit, seat = lax.div(j, share), k * share + lax.rem(j, share)
            start = pl.multiple_of((unit * groups + seat) * LANES, LANES)
            pltpu.make_async_copy(
                table_ref.at[0, :, pl.ds(start, LANES)], blocks.at[unit, seat], sem
            ).start()
            return carry

        lax.fori_loop(0, table_ref.shape[2] // LANES // len(sems), load, 0)


def send_rows(groups, cols, stride, me, own, source, target, send_sem, recv_sem):
    devices = groups * cols

    def send(i, carry):
        to_grp, to_col = peer_of(lax.rem(i * stride, devices), me)
        pltpu.make_async_remote_copy(
            src_ref=source.at[to_grp * cols + to_col],
            dst_ref=target.at[own],
            send_sem=send_sem,
            recv_sem=recv_sem,
            device_id=(to_grp, to_col),
            device_id_type=MESH,
        ).start()
        return carry

    lax.fori_loop(1, devices, send, 0)


def turn_table(groups, blocks, rows_by_id):
    units, _, width, _ = blocks.shape
    table_len = units * groups * LANES

    def turn(j, carry):
        for u in range(4):
            p = lax.rem(j, groups // 4) * 4 + u
            unit = lax.div(j, groups // 4)
            start = pl.multiple_of((unit * groups + p) * LANES, LANES)
            rows_by_id[pl.ds(start, LANES), :] = blocks[unit, p].T.astype(jnp.float32)
        return carry

    lax.fori_loop(0, units * groups // 4, turn, 0)
    rows_by_id[pl.ds(table_len, 8), :] = jnp.zeros((8, width), jnp.float32)


def pool_bags(devices, rows_by_id, ids_in, ids_smem, sums, ids_recv_sem, local_sem):
    wait_for(ids_in.at[pl.ds(0, devices - 1)], ids_recv_sem)
    to_smem = pltpu.make_async_copy(ids_in, ids_smem, local_sem)
    to_smem.start()
    to_smem.wait()
    samples = sums.shape[1]

    def pool(d, carry):
        for b in range(samples):
            terms = [rows_by_id[pl.ds(ids_smem[d, 0, b * BAG + i], 1), :] for i in range(BAG)]
            while len(terms) > 1:
                terms = [terms[k] + terms[k + 1] for k in range(0, len(terms), 2)]
            sums[d, b : b + 1, :] = terms[0]
        return carry

    lax.fori_loop(0, devices, pool, 0)


def wait_for(ref, sem):
    pltpu.make_async_copy(ref, ref, sem).wait()


def exchange_kernel(
    groups, cols, stride, tables_ref, ids_ref, table_ref, out_ref, ret_ref,
    blocks, landed, packed, rows_by_id, ids_in, ids_smem, sums,
    local_sem, send_sem, recv_sem, send2_sem, recv2_sem,
    ids_send_sem, ids_recv_sem, sum_send_sem, sum_recv_sem,
):
    devices = groups * cols
    width = table_ref.shape[1]
    narrow = width // cols
    grp = lax.axis_index("grp")
    col = lax.axis_index("col")
    own = grp * cols + col
    me = (lax.div(grp, 8), lax.rem(lax.div(grp, 2), 4), lax.rem(grp, 2), col)

    barrier = greet_all(groups, cols, me)
    load_table(groups, table_ref, blocks, (local_sem,))
    pl.semaphore_wait(barrier, devices - 1)
    send_rows(groups, cols, stride, me, own, ids_ref, ids_in, ids_send_sem, ids_recv_sem)
    ids_in[own] = ids_ref[own]
    wait_for(blocks, local_sem)

    def send(i, carry):
        offset = lax.rem(i * stride, devices)
        to_grp, to_col = peer_of(offset, me)
        pltpu.make_async_remote_copy(
            src_ref=blocks.at[:, to_grp, pl.ds(pl.multiple_of(to_col * narrow, narrow), narrow), :],
            dst_ref=landed.at[own],
            send_sem=send_sem,
            recv_sem=recv_sem,
            device_id=(to_grp, to_col),
            device_id_type=MESH,
        ).start()
        return carry

    lax.fori_loop(1, devices, send, 0)
    landed[own] = blocks[:, grp, pl.ds(pl.multiple_of(col * narrow, narrow), narrow), :]

    turn_table(groups, blocks, rows_by_id)
    pool_bags(devices, rows_by_id, ids_in, ids_smem, sums, ids_recv_sem, local_sem)
    send_rows(groups, cols, stride, me, own, sums, ret_ref, sum_send_sem, sum_recv_sem)
    own_sums = pltpu.make_async_copy(sums.at[own], ret_ref.at[own], local_sem)
    own_sums.start()
    own_sums.wait()
    everyone = landed.at[pl.ds(0, devices - 1)]
    wait_for(everyone, recv_sem)

    per_group = packed.shape[1]

    def pack(j, carry):
        slot = tables_ref[SLOTS, j]
        count = tables_ref[COUNTS, j]
        block = landed[slot]
        unit = lax.broadcasted_iota(jnp.int32, block.shape, 0)
        packed[lax.div(j, per_group), lax.rem(j, per_group)] = jnp.where(
            unit < count, block, jnp.zeros_like(block)
        )
        return carry

    lax.fori_loop(0, groups * per_group, pack, 0)

    def send2(i, carry):
        offset = lax.rem(lax.rem(i, groups - 1) + 1, groups) * 27
        q = lax.div(i, groups - 1)
        to_grp, _ = peer_of(lax.rem(offset, groups), me)
        pltpu.make_async_remote_copy(
            src_ref=packed.at[to_grp, q],
            dst_ref=out_ref.at[grp, q],
            send_sem=send2_sem,
            recv_sem=recv2_sem,
            device_id=(to_grp, col),
            device_id_type=MESH,
        ).start()
        return carry

    lax.fori_loop(0, per_group * (groups - 1), send2, 0)
    mine = pltpu.make_async_copy(packed.at[grp], out_ref.at[grp], local_sem)
    mine.start()
    mine.wait()
    wait_for(everyone, send_sem)
    wait_for(packed.at[pl.ds(0, groups - 1)], send2_sem)
    wait_for(out_ref.at[pl.ds(0, groups - 1)], recv2_sem)
    wait_for(ids_in.at[pl.ds(0, devices - 1)], ids_send_sem)
    wait_for(sums.at[pl.ds(0, devices - 1)], sum_send_sem)
    wait_for(ret_ref.at[pl.ds(0, devices - 1)], sum_recv_sem)


def exchange(tables, ids, old_tables, groups, cols, stride=37):
    _, width, table_len = old_tables.shape
    devices = groups * cols
    narrow = width // cols
    per_group = tables.shape[1] // groups
    column_blocks = table_len // LANES
    units = column_blocks // groups
    dtype = old_tables.dtype
    samples = LANES // BAG
    return pl.pallas_call(
        functools.partial(exchange_kernel, groups, cols, stride),
        out_shape=(
            jax.ShapeDtypeStruct((groups, per_group, units, narrow, LANES), dtype),
            jax.ShapeDtypeStruct((devices, samples, width), jnp.float32),
        ),
        in_specs=[
            pl.BlockSpec(memory_space=pltpu.SMEM),
            pl.BlockSpec(memory_space=pltpu.VMEM),
            pl.BlockSpec(memory_space=pl.ANY),
        ],
        out_specs=(pl.BlockSpec(memory_space=pl.ANY), pl.BlockSpec(memory_space=pl.ANY)),
        scratch_shapes=[
            pltpu.VMEM((units, groups, width, LANES), dtype),
            pltpu.VMEM((devices, units, narrow, LANES), dtype),
            pltpu.VMEM((groups, per_group, units, narrow, LANES), dtype),
            pltpu.VMEM((table_len + 8, width), jnp.float32),
            pltpu.VMEM((devices, 1, LANES), jnp.int32),
            pltpu.SMEM((devices, 1, LANES), jnp.int32),
            pltpu.VMEM((devices, samples, width), jnp.float32),
        ]
        + [pltpu.SemaphoreType.DMA] * 9,
        compiler_params=pltpu.CompilerParams(
            collective_id=LEVELS_ID, has_side_effects=True, vmem_limit_bytes=60 * 1024 * 1024
        ),
        name="exchange",
    )(tables, ids, old_tables)


def route_kernel(
    groups, cols, stride, cap2, cap3, hold, chunks,
    tables_ref, ids_ref, table_ref, out_ref, ret_ref,
    blocks, rows_by_id, ids_in, ids_smem, sums, first, outgoing, second, final,
    local_sem, late_sem, ids_send_sem, ids_recv_sem, sum_send_sem, sum_recv_sem,
    send1_sem, recv1_sem, send2_sem, recv2_sem, send3_sem, recv3_sem, own3_sem,
):
    devices = groups * cols
    width = blocks.shape[2]
    narrow = width // cols
    piece = first[0].shape[1]
    parts = narrow // piece
    grp = lax.axis_index("grp")
    col = lax.axis_index("col")
    own = grp * cols + col
    y, x, core = lax.div(grp, 8), lax.rem(lax.div(grp, 2), 4), lax.rem(grp, 2)
    me = (y, x, core, col)
    along = (y, x)
    across = (x, y)
    line = 8
    source = [(along[h] * 2 + core) * cols + col for h in range(2)]
    seat = [along[h] * 2 + core for h in range(2)]

    def at(h, u, v, c):
        return ((u * 4 + v) * 2 + c) if h == 0 else ((v * 4 + u) * 2 + c)

    barrier = greet_all(groups, cols, me)
    near, far = (blocks.at[:, pl.ds(k * groups // 2, groups // 2)] for k in range(2))
    load_table(groups, table_ref, blocks, (local_sem, late_sem))
    pl.semaphore_wait(barrier, devices - 1)
    wait_for(near, local_sem)

    def ids_out():
        send_rows(groups, cols, stride, me, own, ids_ref, ids_in, ids_send_sem, ids_recv_sem)
        ids_in[own] = ids_ref[own]

    def turn():
        wait_for(far, late_sem)
        turn_table(groups, blocks, rows_by_id)

    def stage1(n, sides=(0, 1)):
        c, w = n // parts, n % parts

        def send(i, carry):
            o = lax.rem(i * 5, 32)
            dc, du, dz = lax.rem(o, 2), lax.rem(lax.div(o, 2), 4), lax.div(o, 8)
            tz = lax.rem(col + dz, 4)
            tc = lax.rem(core + dc, 2)
            start = pl.multiple_of(tz * narrow + w * piece, piece)
            for h in sides:
                tu = lax.rem(along[h] + du, 4)
                pltpu.make_async_remote_copy(
                    src_ref=blocks.at[:, h * 16 + c * 8 + tu * 2 + tc, pl.ds(start, piece), :],
                    dst_ref=first[h * chunks + n].at[pl.ds(source[h] * 8, 8)],
                    send_sem=send1_sem.at[h * chunks + n],
                    recv_sem=recv1_sem.at[h * chunks + n],
                    device_id=(at(h, tu, across[h], tc), tz),
                    device_id_type=MESH,
                ).start()
            return carry

        lax.fori_loop(1, 32, send, 0)
        start = pl.multiple_of(col * narrow + w * piece, piece)
        for h in sides:
            first[h * chunks + n][pl.ds(source[h] * 8, 8)] = blocks[
                :, h * 16 + c * 8 + seat[h], pl.ds(start, piece), :
            ]

    def arrived1(n, sides=(0, 1)):
        for h in sides:
            i = h * chunks + n
            wait_for(first[i].at[pl.ds(0, 31 * 8)], recv1_sem.at[i])

    def stage2(n, sides=(0, 1)):
        half = cap2 // 2
        for h in sides:
            i = h * chunks + n

            def pack(m, carry):
                for dv in range(1, 4):
                    for u in range(4):
                        outgoing[i][(dv - 1) * cap2 + m * 4 + u] = first[i][
                            tables_ref[h * 4 + dv, m * 4 + u]
                        ]
                return carry

            lax.fori_loop(0, cap2 // 4, pack, 0)
            for m in range(2):
                for dv in (1, 3, 2):
                    pltpu.make_async_remote_copy(
                        src_ref=outgoing[i].at[pl.ds((dv - 1) * cap2 + m * half, half)],
                        dst_ref=second[i].at[pl.ds(dv * hold + m * half, half)],
                        send_sem=send2_sem.at[i],
                        recv_sem=recv2_sem.at[i],
                        device_id=(at(h, along[h], lax.rem(across[h] + dv, 4), core), col),
                        device_id_type=MESH,
                    ).start()
        for h in sides:
            i = h * chunks + n

            def keep(m, carry):
                for u in range(4):
                    second[i][m * 4 + u] = first[i][tables_ref[h * 4, m * 4 + u]]
                return carry

            lax.fori_loop(0, hold // 4, keep, 0)

    def stage3(n, sides=(0, 1)):
        for h in sides:
            i = h * chunks + n
            wait_for(second[i].at[pl.ds(0, 3 * cap2)], recv2_sem.at[i])

            def pack(m, carry):
                for d in range(line):
                    final[i][d, m] = second[i][tables_ref[LISTS3 + h * line + d, m]]
                return carry

            lax.fori_loop(0, cap3, pack, 0)
            for d in (5, 3, 7, 2, 6, 4, 1):
                tu = lax.rem(along[h] + d // 2, 4)
                tc = lax.rem(core + d % 2, 2)
                pltpu.make_async_remote_copy(
                    src_ref=final[i].at[d],
                    dst_ref=out_ref.at[h, n, seat[h]],
                    send_sem=send3_sem.at[i],
                    recv_sem=recv3_sem.at[i],
                    device_id=(at(h, tu, across[h], tc), col),
                    device_id_type=MESH,
                ).start()
            pltpu.make_async_copy(final[i].at[0], out_ref.at[h, n, seat[h]], own3_sem.at[i]).start()

    def bags():
        pool_bags(devices, rows_by_id, ids_in, ids_smem, sums, ids_recv_sem, local_sem)

    def sums_out():
        send_rows(groups, cols, stride, me, own, sums, ret_ref, sum_send_sem, sum_recv_sem)
        pltpu.make_async_copy(sums.at[own], ret_ref.at[own], local_sem).start()

    for stage, n in ORDER:
        steps = (
            bags, ids_out, turn, sums_out, stage1, arrived1, stage2, stage3,
        )
        steps[stage](*(() if stage < 4 else (n // 3, ((0,), (1,), (0, 1))[n % 3])))
    for h in range(2):
        for n in range(chunks):
            i = h * chunks + n
            wait_for(first[i].at[pl.ds(0, 31 * 8)], send1_sem.at[i])
            wait_for(outgoing[i], send2_sem.at[i])
            wait_for(final[i].at[pl.ds(0, line - 1)], send3_sem.at[i])
            wait_for(final[i].at[0], own3_sem.at[i])
            wait_for(out_ref.at[h, n, pl.ds(0, line - 1)], recv3_sem.at[i])
    wait_for(sums.at[own], local_sem)
    wait_for(ids_in.at[pl.ds(0, devices - 1)], ids_send_sem)
    wait_for(sums.at[pl.ds(0, devices - 1)], sum_send_sem)
    wait_for(ret_ref.at[pl.ds(0, devices - 1)], sum_recv_sem)


def routed(tables, ids, old_tables, groups, cols, cap2, cap3, number, chunks=CHUNKS, stride=37):
    _, width, table_len = old_tables.shape
    devices = groups * cols
    piece = (width // cols) * 2 // chunks
    units = table_len // LANES // groups
    dtype = old_tables.dtype
    samples = LANES // BAG
    smem = pl.BlockSpec(memory_space=pltpu.SMEM)
    hbm = pl.BlockSpec(memory_space=pl.ANY)
    both = 2 * chunks
    dma = pltpu.SemaphoreType.DMA
    return pl.pallas_call(
        functools.partial(route_kernel, groups, cols, stride, cap2, cap3, HOLD, chunks),
        out_shape=(
            jax.ShapeDtypeStruct((2, chunks, 8, cap3, piece, LANES), dtype),
            jax.ShapeDtypeStruct((devices, samples, width), jnp.float32),
        ),
        in_specs=[smem, pl.BlockSpec(memory_space=pltpu.VMEM), hbm],
        out_specs=(hbm, hbm),
        scratch_shapes=[
            pltpu.VMEM((units, groups, width, LANES), dtype),
            pltpu.VMEM((table_len + 8, width), jnp.float32),
            pltpu.VMEM((devices, 1, LANES), jnp.int32),
            pltpu.SMEM((devices, 1, LANES), jnp.int32),
            pltpu.VMEM((devices, samples, width), jnp.float32),
            [pltpu.VMEM((devices // 4 * units, piece, LANES), dtype) for _ in range(both)],
            [pltpu.VMEM((3 * cap2, piece, LANES), dtype) for _ in range(both)],
            [pltpu.VMEM((4 * HOLD, piece, LANES), dtype) for _ in range(both)],
            [pltpu.VMEM((8, cap3, piece, LANES), dtype) for _ in range(both)],
        ]
        + [dma] * 6
        + [dma((both,))] * 7,
        compiler_params=pltpu.CompilerParams(
            collective_id=number, has_side_effects=True, vmem_limit_bytes=63 * 1024 * 1024
        ),
        name="routed",
    )(tables, ids, old_tables)


def plan_kernel(
    old_ref, new_ref, rows_ref, ids_ref, len_ref, tables_ref, level_ref, ids_out, turned
):
    samples, size = len_ref.shape
    grp = lax.axis_index("grp")
    y, x, core = lax.div(grp, 8), lax.rem(lax.div(grp, 2), 4), lax.rem(grp, 2)
    down = lax.broadcasted_iota(jnp.int32, (size, size), 0)
    lane = lax.broadcasted_iota(jnp.int32, (size, size), 1)
    index = lax.broadcasted_iota(jnp.int32, (1, size), 1)

    def column(row):
        return jnp.broadcast_to(row, (size, size)).T

    def total(mask, value):
        return jnp.sum(jnp.where(mask, value, 0), axis=0, keepdims=True)

    def put(row, value):
        tables_ref[row : row + 1, :] = value

    old_down = column(old_ref[...])
    new = new_ref[...]
    slot = total(old_down == new, down)
    count = total(down == new, column(rows_ref[...] // UNIT))
    put(SLOTS, slot)
    put(COUNTS, count)
    put(INVERSE, total(old_down == lane, down))
    count_down = column(count)
    target_down = down // 4
    base = total((target_down == index // 4) & (down < lane), count_down)
    base_down = column(base)
    slot_down = column(slot)
    core_from, z_from = (slot_down // 4) % 2, slot_down % 4
    core_to = target_down % 2
    sides = []
    for place_down, place in ((slot_down // 4, slot // 4), (target_down, index // 4)):
        sides.append(((place_down // 8, (place_down // 2) % 4), (place // 8, (place // 2) % 4)))
    need0 = need2 = jnp.zeros((1, 1), jnp.int32)
    for h, (u, v) in enumerate(((y, x), (x, y))):
        u_from, v_from = sides[0][0][h], sides[0][0][1 - h]
        u_to, v_to = sides[1][0][h], sides[1][0][1 - h]
        pair_down = v_from * 4 + v_to
        pair = sides[0][1][1 - h] * 4 + sides[1][1][1 - h]
        begun = total((pair_down == pair) & (down < lane), count_down)
        begun_down = column(begun)
        sums = total(pair_down == lane, count_down)
        same = index % 5 == 0
        need0 = jnp.maximum(need0, jnp.max(jnp.where(same, sums, 0), axis=1, keepdims=True))
        need2 = jnp.maximum(need2, jnp.max(jnp.where(same, 0, sums), axis=1, keepdims=True))
        step = (v_to - v_from + 4) % 4
        source = ((u_from * 2 + core_from) * 4 + z_from) * 8 + lane - begun_down
        inside = (v_from == v) & (lane >= begun_down) & (lane < begun_down + count_down)
        for dv in range(4):
            put(h * 4 + dv, total(inside & (step == dv), source))
        rel = ((u_to - u + 4) % 4) * 2 + (core_to - core + 2) % 2
        held = step * HOLD + jnp.minimum(begun_down + lane - base_down, HOLD - 1)
        inside = (v_to == v) & (lane >= base_down) & (lane < base_down + count_down)
        for d in range(8):
            put(LISTS3 + h * 8 + d, total(inside & (rel == d), held))
    need3 = jnp.max(total(target_down == lane, count_down), axis=1, keepdims=True)
    level = jnp.full((1, 1), len(LEVELS), jnp.int32)
    for number in reversed(range(len(LEVELS))):
        cap2, cap3 = LEVELS[number]
        fits = (need0 <= HOLD) & (need2 <= cap2) & (need3 <= cap3)
        level = jnp.where(fits, number, level)
    level_ref[0] = level[0, 0]
    mine = total(down == grp * 4 + lane, count_down)
    offset = total(down == grp * 4 + lane - 4, base_down)
    put(MINE, jnp.where(index < 4, mine, offset))

    turn_in = lax.broadcasted_iota(jnp.int32, (BAG, size), 0)
    parts = []
    for b in range(samples):
        used = turn_in < len_ref[b : b + 1, :]
        parts.append(jnp.where(used, ids_ref[b * BAG : (b + 1) * BAG, :], ROWS))
    flat = jnp.concatenate(parts, axis=0).T
    high = jnp.dot(
        (old_down == lane).astype(jnp.bfloat16), (flat // 256).astype(jnp.bfloat16),
        preferred_element_type=jnp.float32,
    )
    low = jnp.dot(
        (old_down == lane).astype(jnp.bfloat16), (flat % 256).astype(jnp.bfloat16),
        preferred_element_type=jnp.float32,
    )
    turned[...] = high.astype(jnp.int32) * 256 + low.astype(jnp.int32)

    def copy(s, carry):
        for i in range(8):
            ids_out[s * 8 + i] = turned[pl.ds(s * 8 + i, 1), :]
        return carry

    lax.fori_loop(0, size // 8, copy, 0)


def plan(old_plan, new_plan, table_rows, ids, bag_len):
    tables = old_plan.shape[0]
    vmem = pl.BlockSpec(memory_space=pltpu.VMEM)
    flat = jnp.transpose(ids, (0, 2, 1)).reshape(-1, tables)
    return pl.pallas_call(
        plan_kernel,
        out_shape=(
            jax.ShapeDtypeStruct((32, tables), jnp.int32),
            jax.ShapeDtypeStruct((1,), jnp.int32),
            jax.ShapeDtypeStruct((tables, 1, flat.shape[0]), jnp.int32),
        ),
        in_specs=[vmem] * 5,
        out_specs=(vmem, pl.BlockSpec(memory_space=pltpu.SMEM), vmem),
        scratch_shapes=[pltpu.VMEM((tables, flat.shape[0]), jnp.int32)],
        name="plan",
    )(old_plan[None], new_plan[None], table_rows[None], flat, bag_len)


def reorder_sums(share, tables_ref, ret_ref, pooled_ref):
    samples = pooled_ref.shape[0]
    first = (pl.program_id(0) * pl.num_programs(1) + pl.program_id(1)) * share

    def reorder(i, carry):
        table = first + i
        rows = ret_ref[tables_ref[INVERSE, table]]
        for b in range(samples):
            pooled_ref[b, pl.ds(table, 1), :] = rows[b : b + 1, :]
        return carry

    lax.fori_loop(0, share, reorder, 0)


def unpack_kernel(steps, tables_ref, in_ref, ret_ref, out_ref, pooled_ref):
    groups, _, units = in_ref.shape[:3]
    for k in range(units):
        for p in range(groups):
            start = (k * groups + p) * LANES
            out_ref[0, :, start : start + LANES] = in_ref[p, 0, k]
    reorder_sums(tables_ref.shape[1] // steps, tables_ref, ret_ref, pooled_ref)


def unpack_routed_kernel(
    tables_ref, in_ref, ret_in_ref, out_ref, pooled_ref, taken, built, ret, in_sem, ret_sem, out_sem
):
    halves, chunks, seats, cap3, piece, lanes = in_ref.shape
    per_group, narrow, table_len = out_ref.shape
    parts = narrow // piece
    units = table_len // UNIT
    tables = ret.shape[0]
    samples = ret.shape[1]
    split = 2
    fetched = pltpu.make_async_copy(ret_in_ref, ret, ret_sem)

    def take(q, k):
        where = jnp.minimum(tables_ref[MINE, 4 + q] + k, cap3 - 1)
        return pltpu.make_async_copy(in_ref.at[:, :, :, where], taken.at[q, k], in_sem.at[q, k])

    for q in range(per_group):

        def ask(k, carry):
            @pl.when(k < tables_ref[MINE, q])
            def _():
                take(q, k).start()

            return carry

        lax.fori_loop(0, units, ask, 0)
    fetched.start()

    def put_out(q, r):
        size = table_len // split
        return pltpu.make_async_copy(
            built.at[q, :, pl.ds(r * size, size)], out_ref.at[q, :, pl.ds(r * size, size)],
            out_sem.at[q * split + r],
        )

    for q in range(per_group):
        count = tables_ref[MINE, q]
        for r in range(split):

            def build(k, carry):
                begin = pl.multiple_of(k * UNIT, UNIT)

                @pl.when(k < count)
                def _():
                    take(q, k).wait()
                    for h in range(halves):
                        for n in range(chunks):
                            c, w = n // parts, n % parts
                            for p in range(seats):
                                start = begin + (h * 16 + c * 8 + p) * lanes
                                built[q, w * piece : (w + 1) * piece, pl.ds(start, lanes)] = taken[
                                    q, k, h, n, p
                                ]

                @pl.when(k >= count)
                def _():
                    built[q, :, pl.ds(begin, UNIT)] = jnp.zeros((narrow, UNIT), built.dtype)

                return carry

            lax.fori_loop(r * units // split, (r + 1) * units // split, build, 0)
            put_out(q, r).start()
    fetched.wait()

    def reorder(i, carry):
        for u in range(4):
            rows = ret[tables_ref[INVERSE, i * 4 + u]]
            for b in range(samples):
                pooled_ref[b, pl.ds(i * 4 + u, 1), :] = rows[b : b + 1, :]
        return carry

    lax.fori_loop(0, tables // 4, reorder, 0)
    for q in range(per_group):
        for r in range(split):
            put_out(q, r).wait()


def unpack_routed(tables, received, returned, narrow, table_len):
    halves, chunks, seats, _, piece, lanes = received.shape
    devices, samples, width = returned.shape
    hbm = pl.BlockSpec(memory_space=pl.ANY)
    units = table_len // UNIT
    dma = pltpu.SemaphoreType.DMA
    return pl.pallas_call(
        unpack_routed_kernel,
        out_shape=(
            jax.ShapeDtypeStruct((4, narrow, table_len), received.dtype),
            jax.ShapeDtypeStruct((samples, devices, width), returned.dtype),
        ),
        in_specs=[pl.BlockSpec(memory_space=pltpu.SMEM), hbm, hbm],
        out_specs=(hbm, pl.BlockSpec(memory_space=pltpu.VMEM)),
        scratch_shapes=[
            pltpu.VMEM((4, units, halves, chunks, seats, piece, lanes), received.dtype),
            pltpu.VMEM((4, narrow, table_len), received.dtype),
            pltpu.VMEM(returned.shape, returned.dtype),
            dma((4, units)),
            dma,
            dma((8,)),
        ],
        compiler_params=pltpu.CompilerParams(vmem_limit_bytes=62 * 1024 * 1024),
        name="unpack_routed",
    )(tables, received, returned)


def unpack(kernel, block, index, tables, received, returned, narrow, table_len, step=4):
    devices, samples, width = returned.shape
    per_group = 4
    splits = table_len // UNIT // step
    smem = pl.BlockSpec(memory_space=pltpu.SMEM)
    return pl.pallas_call(
        functools.partial(kernel, per_group * splits),
        out_shape=(
            jax.ShapeDtypeStruct((per_group, narrow, table_len), received.dtype),
            jax.ShapeDtypeStruct((samples, devices, width), returned.dtype),
        ),
        grid=(per_group, splits),
        in_specs=[
            smem,
            pl.BlockSpec(block, index),
            pl.BlockSpec((devices, samples, width), lambda q, k: (0, 0, 0)),
        ],
        out_specs=(
            pl.BlockSpec((1, narrow, step * UNIT), lambda q, k: (q, 0, k)),
            pl.BlockSpec((samples, devices, width), lambda q, k: (0, 0, 0)),
        ),
        compiler_params=pltpu.CompilerParams(vmem_limit_bytes=40 * 1024 * 1024),
        name="unpack",
    )(tables, received, returned)


def body(old_tables, table_rows, old_plan, new_plan, ids, bag_len):
    groups = lax.axis_size("grp")
    cols = lax.axis_size("col")
    _, width, table_len = old_tables.shape
    narrow = width // cols
    tables, level, own_ids = plan(old_plan, new_plan, table_rows, ids, bag_len)

    def by_level(number):
        cap2, cap3 = LEVELS[number]

        def run():
            received, returned = routed(
                tables, own_ids, old_tables, groups, cols, cap2, cap3, number
            )
            return unpack_routed(tables, received, returned, narrow, table_len)

        return run

    def spread():
        received, returned = exchange(tables, own_ids, old_tables, groups, cols)
        block = received.shape[:1] + (1, 4) + received.shape[3:]
        return unpack(
            unpack_kernel, block, lambda q, k: (0, q, k, 0, 0),
            tables, received, returned, narrow, table_len,
        )

    branches = [by_level(number) for number in range(len(LEVELS))] + [spread]
    return lax.switch(level.reshape(()), branches)


def solution(mesh):
    return jax.shard_map(
        body,
        mesh=mesh,
        in_specs=(
            P(("grp", "col"), None, None),
            P(),
            P(),
            P(),
            P(("grp", "col"), None, None),
            P(("grp", "col"), None),
        ),
        out_specs=(P("grp", "col", None), P(("grp", "col"), None, None)),
        check_vma=False,
    )
```
